128 devices in a mesh: section: 4 (over x_lo, core), tensor: 32 (over z, x_hi, y).
Axes of the slice: x: 4 (x_hi: 2, x_lo: 2; x = x_hi * 2 + x_lo), y: 4, z: 4, core: 2. Of those that a mesh axis runs over, the one named last changes fastest.
Arguments:
- tokens: bfloat16 [2, 64, 4096], replicated, may hold values from -6 to 6
- norm_gain: bfloat16 [4, 4096], replicated, may hold values from 0.25 to 1.75
- w_in: bfloat16 [4, 2, 14336, 4096], P('section', None, 'tensor'), may hold values from -0.09375 to 0.09375
- w_out: bfloat16 [4, 14336, 4096], P('section', 'tensor'), may hold values from -0.046875 to 0.046875
- backup_in: bfloat16 [4, 2, 14336, 4096], P('section', None, 'tensor'), may hold values from -0.09375 to 0.09375
- backup_out: bfloat16 [4, 14336, 4096], P('section', None, 'tensor'), may hold values from -0.046875 to 0.046875
- layer_group: int32 [4], replicated, may hold values from 0 to 3, as said below
- token_counts: int32 [2], replicated, may hold values from 1 to 64, as said below
Outputs:
- handed: bfloat16 [4, 2, 64, 4096], P('section', None, 'tensor')
The draws below stay inside these ranges and needn't reach their ends.
Inputs may be any that keep to these rules, and one draw needn't show every extreme that they name: layer_group[l] is l or l + 1. The layers that move up form one run of consecutive layers, at least one, that starts at the layer of the one group left without any layer; that group is never the last one. `token_counts`: rows of a micro-batch from its count on are padding. One micro-batch is full, with 64 real tokens; the other has at most 32.
All inputs are finite; a program needn't handle non-finite values.
Results may differ from the reference program's by a relative error of at most 0.025.
Values may be sent and summed in bfloat16 or wider, within the bound.
A program may use at most 128 MiB of HBM per device.

```python
import jax
import jax.numpy as jnp
from jax import lax

D = 4096
FF = 14336
TOK = 64
MB = 2
LAYERS = 4
BLOCKS = 32


def draw_layer_group(key, part):
    key_lost, key_span = jax.random.split(jax.random.fold_in(key, 7))
    lost_group = jax.random.randint(key_lost, (), 0, LAYERS - 1)
    span_count = 1 + jax.random.randint(key_span, (), 0, LAYERS - 1 - lost_group)
    levels = jnp.arange(LAYERS, dtype=jnp.int32)
    moved_up = (levels >= lost_group) & (levels < lost_group + span_count)
    return levels + moved_up.astype(jnp.int32)


def draw_token_counts(key, part):
    key_low, key_flip = jax.random.split(jax.random.fold_in(key, 11))
    high_count = jnp.int32(TOK)
    low_count = jax.random.randint(key_low, (), 1, TOK // 2 + 1)
    flipped = jax.random.randint(key_flip, (), 0, 2)
    first = jnp.where(flipped == 1, low_count, high_count)
    second = jnp.where(flipped == 1, high_count, low_count)
    return jnp.stack([first, second]).astype(jnp.int32)


def block_levels(key, shape, cuts, smallest, high):
    gain, own = 1.0, jax.random.fold_in(key, 6)
    for dim, parts in cuts:
        steps = jnp.exp(jax.random.uniform(jax.random.fold_in(own, dim), (parts,), jnp.float32, smallest / len(cuts), high / len(cuts)))
        gain = gain * jnp.repeat(steps, shape[dim] // parts).reshape([-1 if axis == dim else 1 for axis in range(len(shape))])
    return gain


def gaussian(stream_key, extent, scale, reach, cuts=(), kind=jnp.bfloat16):
    result = jax.random.normal(stream_key, extent, jnp.float32) * scale
    if len(cuts) > 0:
        result = block_levels(stream_key, extent, cuts, -0.22, 0.18) * result
    return jnp.clip(result, min=-reach, max=reach).astype(kind)


def setup_inputs(seed: int = 0) -> dict:
    splits = jax.random.split(jax.random.key(seed), 9)
    tokens = gaussian(splits[0], (MB, TOK, D), 1.0, 6.0)
    norm_gain = jnp.clip(1.0 + 0.15 * jax.random.normal(splits[1], (LAYERS, D), jnp.float32), 0.25, 1.75).astype(jnp.bfloat16)
    w_in = gaussian(splits[2], (LAYERS, 2, FF, D), D ** -0.5, 0.09375, ((0, 4), (2, 32)))
    w_out = gaussian(splits[3], (LAYERS, FF, D), FF ** -0.5, 0.046875, ((0, 4), (1, 32)))
    backup_in = gaussian(splits[4], (LAYERS, 2, FF, D), D ** -0.5, 0.09375, ((0, 4), (2, 32)))
    backup_out = gaussian(splits[5], (LAYERS, FF, D), FF ** -0.5, 0.046875, ((0, 4), (2, 32)))
    layer_group = draw_layer_group(jax.random.fold_in(splits[8], 71), 0)
    token_counts = draw_token_counts(jax.random.fold_in(splits[8], 71), 0)
    return {"tokens": tokens, "norm_gain": norm_gain, "w_in": w_in, "w_out": w_out, "backup_in": backup_in, "backup_out": backup_out, "layer_group": layer_group, "token_counts": token_counts}


NORM_EPS = 0.25

def apply_layer(current, gain_row, w_pair, w_down, row_keep):
    wide_x = current.astype(jnp.float32)
    mean_square = lax.optimization_barrier(jnp.mean(wide_x * wide_x, axis=1, keepdims=True))
    normed = (wide_x * lax.rsqrt(mean_square + NORM_EPS) * gain_row.astype(jnp.float32)).astype(jnp.bfloat16)
    gate_part = lax.dot_general(normed, w_pair[0], (((1,), (1,)), ((), ())), preferred_element_type=jnp.float32)
    up_part = lax.dot_general(normed, w_pair[1], (((1,), (1,)), ((), ())), preferred_element_type=jnp.float32)
    hidden = (jax.nn.silu(gate_part) * up_part).astype(jnp.bfloat16)
    row_count = hidden.shape[0]
    block_width = FF // BLOCKS
    hidden_blocks = hidden.reshape(row_count, BLOCKS, block_width).astype(jnp.float32)
    down_blocks = w_down.reshape(BLOCKS, block_width, D).astype(jnp.float32)
    partial_value = jnp.einsum('rbf,bfd->brd', hidden_blocks, down_blocks)
    rounded = lax.optimization_barrier(partial_value.astype(jnp.bfloat16))
    summed = lax.optimization_barrier(jnp.sum(rounded.astype(jnp.float32), axis=0))
    return (wide_x + row_keep * summed).astype(jnp.bfloat16)

def reference(tokens, norm_gain, w_in, w_out, backup_in, backup_out, layer_group, token_counts):
    positions = jnp.arange(TOK, dtype=jnp.int32)
    row_keep = (positions[None, :] < token_counts[:, None]).astype(jnp.float32).reshape(MB * TOK, 1)
    current = tokens.reshape(MB * TOK, D)
    history = [current]
    for level in range(LAYERS):
        moved = layer_group[level] == level + 1
        spare = (level + 1) % LAYERS
        pair = jnp.where(moved, backup_in[spare], w_in[level])
        down = jnp.where(moved, backup_out[spare], w_out[level])
        current = apply_layer(current, norm_gain[level][None, :], pair, down, row_keep)
        history.append(current)
    stacked = jnp.stack(history).reshape(LAYERS + 1, MB, TOK, D)
    groups = jnp.arange(LAYERS, dtype=jnp.int32)
    reached = lax.optimization_barrier(jnp.sum((layer_group[None, :] <= groups[:, None]).astype(jnp.int32), axis=1))
    return jnp.take(stacked, reached, axis=0)
```

```python
import functools

import jax
import jax.numpy as jnp
from jax import lax
from jax.experimental import pallas as pl
from jax.experimental.pallas import tpu as pltpu
from jax.sharding import Mesh
from jax.sharding import PartitionSpec as P

TENSOR = ("z", "xhi", "y")
AXES = ("section", "z", "xhi", "y")
MESH_ID = pl.DeviceIdType.MESH
NORM_EPS = 0.25
PLANS = ((1, 0, 0), (1, 1, 0), (1, 1, 1), (0, 1, 0), (0, 1, 1), (0, 0, 1))
NZ, NX, NY = 4, 2, 4
NXY = NX * NY
N = NZ * NXY
DZ_ORDER = (0, 1, 3, 2)
FULL, SHORT = 64, 32
ROWS = FULL + SHORT
BLK = 128
UNITS = 448


def hops(d):
    return min(d[0], NZ - d[0]) + 2 * d[1] + min(d[2], NY - d[2])


DISPS = sorted(
    [(a, b, c) for a in range(NZ) for b in range(NX) for c in range(NY)],
    key=lambda d: (-hops(d), d),
)
BACK = [DISPS.index(((-a) % NZ, (-b) % NX, (-c) % NY)) for a, b, c in DISPS]


def table(index, values):
    out = jnp.int32(values[-1])
    for k in range(len(values) - 2, -1, -1):
        out = jnp.where(index == k, jnp.int32(values[k]), out)
    return out


def relay_kernel(
    moved,
    counts, tokens, gains, w_in, w_out, b_in, b_out,
    out_ref,
    tok_v, gain_v, wg, wd, xbuf, ps, rs, xs, xsf, orow, accg, accu, ssq,
    tok_sem, wg_sem, wd_sem, rd_send, rs_send, rs_recv, ag_send, ag_recv, o_send, o_recv,
):
    m = tuple(moved) + (0,)
    runs = [l + m[l] for l in range(4)]
    reached = [sum(e <= g for e in runs) for g in range(4)]
    lost = moved.index(1)
    next_group = [runs[l + 1] if l < 3 else 0 for l in range(4)]
    next_slot = [1 - m[l + 1] if l < 3 else 0 for l in range(4)]
    own_out = [int(reached[runs[l]] == l + 1) for l in range(4)]
    lost_out = [int(lost > 0 and reached[lost] == l + 1) for l in range(4)]
    has_slot = [[int(g > 0 and m[g - 1] == 1) for g in range(4)], [1 - m[g] for g in range(4)]]
    source = [runs[r - 1] if r > 0 else -1 for r in reached]

    sec = lax.axis_index("section")
    z, xh, y = (lax.axis_index(a) for a in TENSOR)
    xy = xh * NY + y
    me = z * NXY + xy

    def at(d):
        return lax.rem(z + d[0], NZ), lax.rem(xh + d[1], NX), lax.rem(y + d[2], NY)

    def flat(p):
        return p[0] * NXY + p[1] * NY + p[2]

    def active(slot):
        return jnp.where(slot == 0, table(sec, has_slot[0]), table(sec, has_slot[1])) == 1

    tok_copy = pltpu.make_async_copy(tokens, tok_v, tok_sem.at[0])
    gain_copy = pltpu.make_async_copy(gains, gain_v, tok_sem.at[1])
    tok_copy.start()
    gain_copy.start()

    def wg_copy(slot, i, half):
        src = w_in if slot == 1 else b_in
        start = pl.multiple_of(lax.rem(z + DZ_ORDER[i], NZ) * (NXY * BLK), NXY * BLK)
        return pltpu.make_async_copy(
            src.at[half, :, pl.ds(start, NXY * BLK)], wg.at[slot, i, half], wg_sem.at[slot, i, half]
        )

    def wd_copy(j):
        start = pl.multiple_of(flat(at(DISPS[j])) * BLK, BLK)
        return pltpu.make_async_copy(w_out.at[:, pl.ds(start, BLK)], wd.at[1, j], wd_sem.at[1, j])

    def redistribute(j):
        to = at(DISPS[j])
        start = pl.multiple_of(flat(to) * UNITS, UNITS)
        src = b_out.at[pl.ds(start, UNITS), :]
        if j == N - 1:
            return pltpu.make_async_copy(src, wd.at[0, j], wd_sem.at[0, j])
        return pltpu.make_async_remote_copy(
            src_ref=src, dst_ref=wd.at[0, BACK[j]], send_sem=rd_send.at[j], recv_sem=wd_sem.at[0, BACK[j]],
            device_id=(sec, *to), device_id_type=MESH_ID,
        )

    for slot in (0, 1):
        @pl.when(table(sec, has_slot[slot]) == 1)
        def _():
            for i in range(NZ):
                for half in range(2):
                    wg_copy(slot, i, half).start()
            if slot == 1:
                for j in range(N):
                    wd_copy(j).start()

    barrier = pltpu.get_barrier_semaphore()

    def greet(k, _):
        g, t = k // N, lax.rem(k, N)

        @pl.when((g != sec) | (t != me))
        def _():
            pl.semaphore_signal(
                barrier, inc=1,
                device_id=(g, t // NXY, lax.rem(t, NXY) // NY, lax.rem(t, NY)), device_id_type=MESH_ID,
            )
        return 0

    lax.fori_loop(0, 4 * N, greet, 0)

    full = jnp.where(counts[1] == FULL, 1, 0)
    short_count = jnp.where(full == 1, counts[0], counts[1])
    tok_copy.wait()
    gain_copy.wait()

    first_slot = 1 - m[0]

    @pl.when(sec == runs[0])
    def _():
        for i in range(NZ):
            zz = lax.rem(z + DZ_ORDER[i], NZ)
            for k in range(NXY):
                cols = pl.ds(pl.multiple_of((zz * NXY + k) * BLK, BLK), BLK)
                xbuf[first_slot, i, k, 0:FULL, :] = tok_v[full, :, cols]
                xbuf[first_slot, i, k, FULL:ROWS, :] = tok_v[1 - full, 0:SHORT, cols]

    pl.semaphore_wait(barrier, 4 * N - 1)

    @pl.when(table(sec, has_slot[0]) == 1)
    def _():
        for j in range(N):
            redistribute(j).start()

    row = lax.broadcasted_iota(jnp.int32, (ROWS, 1), 0)
    keep = jnp.where(row < FULL + short_count, 1.0, 0.0)

    def rs_copy(slot, j):
        return pltpu.make_async_remote_copy(
            src_ref=ps.at[slot, j], dst_ref=rs.at[slot, BACK[j]],
            send_sem=rs_send.at[slot, j], recv_sem=rs_recv.at[slot, BACK[j]],
            device_id=(sec, *at(DISPS[j])), device_id_type=MESH_ID,
        )

    def rs_arrived(slot, j):
        pltpu.make_async_copy(rs.at[slot, j], rs.at[slot, j], rs_recv.at[slot, j]).wait()

    def ag_copy(slot, to_group, to_slot, j):
        d = DISPS[j]
        i = DZ_ORDER.index((-d[0]) % NZ)
        return pltpu.make_async_remote_copy(
            src_ref=xs.at[slot], dst_ref=xbuf.at[to_slot, i, xy],
            send_sem=ag_send.at[slot, j], recv_sem=ag_recv.at[to_slot, i, xy],
            device_id=(to_group, *at(d)), device_id_type=MESH_ID,
        )

    def piece(slot, to_group, which, j, part):
        to = at(DISPS[j])
        first = flat(to) * 2 + (FULL if part else 0)
        return pltpu.make_async_remote_copy(
            src_ref=xsf.at[slot, pl.ds(first, 2)], dst_ref=orow.at[part, me],
            send_sem=o_send.at[slot, which, part, j], recv_sem=o_recv.at[part, me],
            device_id=(to_group, *to), device_id_type=MESH_ID,
        )

    def send_pieces(slot, to_group, which, wait, own):
        for j in range(N):
            short_to = at(DISPS[j])[0] < 2

            def go(copy):
                copy.wait_send() if wait else copy.start()

            if j == N - 1 and own:
                if not wait:
                    orow[0, me] = xsf[slot, pl.ds(me * 2, 2)]

                    @pl.when(short_to)
                    def _():
                        orow[1, me] = xsf[slot, pl.ds(FULL + me * 2, 2)]
            else:
                go(piece(slot, to_group, which, j, 0))

                @pl.when(short_to)
                def _():
                    go(piece(slot, to_group, which, j, 1))

    def layer(slot, _):
        l = sec - 1 + slot
        to_group = table(l, next_group)
        to_slot = table(l, next_slot)
        stays = (to_group == sec) & (l < 3)

        @pl.when(active(slot))
        def _():
            for i in range(NZ):
                zz = lax.rem(z + DZ_ORDER[i], NZ)

                @pl.when(l > 0)
                def _():
                    for k in range(NXY):
                        kept = (slot == 1) & (table(sec, has_slot[0]) == 1) & (k == xy) if i == 0 else None

                        def arrived():
                            pltpu.make_async_copy(
                                xbuf.at[slot, i, k], xbuf.at[slot, i, k], ag_recv.at[slot, i, k]
                            ).wait()

                        if i == 0:
                            pl.when(jnp.logical_not(kept))(arrived)
                        else:
                            arrived()

                for half in range(2):
                    pltpu.make_async_copy(
                        wg.at[slot, i, half], wg.at[slot, i, half], wg_sem.at[slot, i, half]
                    ).wait()
                gain_all = gain_v[:, pl.ds(pl.multiple_of(zz * (NXY * BLK), NXY * BLK), NXY * BLK)].astype(jnp.float32)
                which = lax.broadcasted_iota(jnp.int32, (4, 1), 0)
                gain = jnp.sum(jnp.where(which == l, gain_all, 0.0), axis=0, keepdims=True)
                squares = jnp.zeros((ROWS, BLK), jnp.float32)
                parts = []
                for k in range(NXY):
                    xf = xbuf[slot, i, k].astype(jnp.float32)
                    squares += xf * xf
                    parts.append((xf * gain[:, k * BLK:(k + 1) * BLK]).astype(jnp.bfloat16))
                lhs = jnp.concatenate(parts, axis=1)
                dims = (((1,), (1,)), ((), ()))
                g = lax.dot_general(lhs, wg[slot, i, 0], dims, preferred_element_type=jnp.float32)
                u = lax.dot_general(lhs, wg[slot, i, 1], dims, preferred_element_type=jnp.float32)
                if i == 0:
                    accg[...], accu[...], ssq[...] = g, u, squares
                else:
                    accg[...] += g
                    accu[...] += u
                    ssq[...] += squares
            mean = jnp.sum(ssq[...], axis=1, keepdims=True) * (1.0 / (N * BLK))
            scale = lax.rsqrt(mean + NORM_EPS)
            gate = accg[...] * scale
            hidden = (gate / (1.0 + jnp.exp(-gate)) * (accu[...] * scale)).astype(jnp.bfloat16)

            for j in range(0, N, 2):
                for q in (j, j + 1):
                    pltpu.make_async_copy(wd.at[slot, q], wd.at[slot, q], wd_sem.at[slot, q]).wait()
                w2 = jnp.concatenate([wd[slot, j], wd[slot, j + 1]], axis=1)
                part = jnp.dot(hidden, w2, preferred_element_type=jnp.float32).astype(jnp.bfloat16)
                for q in (j, j + 1):
                    ps[slot, q] = part[:, (q - j) * BLK:(q - j + 1) * BLK]
                    if q < N - 1:
                        rs_copy(slot, q).start()
            total = ps[slot, N - 1].astype(jnp.float32)
            for j in range(N - 2, -1, -1):
                rs_arrived(slot, j)
                total += rs[slot, j].astype(jnp.float32)
            new = (xbuf[slot, 0, xy].astype(jnp.float32) + keep * total).astype(jnp.bfloat16)
            xs[slot] = new
            xsf[slot] = new.astype(jnp.float32).reshape(ROWS, 1, BLK)

            @pl.when(l < 3)
            def _():
                for j in range(N - 1):
                    ag_copy(slot, to_group, to_slot, j).start()

                @pl.when(stays)
                def _():
                    xbuf[1, 0, xy] = new

                @pl.when(jnp.logical_not(stays))
                def _():
                    ag_copy(slot, to_group, to_slot, N - 1).start()

            @pl.when(table(l, own_out) == 1)
            def _():
                send_pieces(slot, sec, 0, False, True)

            if lost > 0:
                @pl.when(table(l, lost_out) == 1)
                def _():
                    send_pieces(slot, jnp.int32(lost), 1, False, False)
        return 0

    lax.fori_loop(0, 2, layer, 0)

    def drain(slot, _):
        l = sec - 1 + slot
        to_group = table(l, next_group)
        to_slot = table(l, next_slot)
        stays = (to_group == sec) & (l < 3)

        @pl.when(active(slot))
        def _():
            for j in range(N - 1):
                rs_copy(slot, j).wait_send()

            @pl.when(l < 3)
            def _():
                for j in range(N - 1):
                    ag_copy(slot, to_group, to_slot, j).wait_send()

                @pl.when(jnp.logical_not(stays))
                def _():
                    ag_copy(slot, to_group, to_slot, N - 1).wait_send()

            @pl.when(table(l, own_out) == 1)
            def _():
                send_pieces(slot, sec, 0, True, True)

            if lost > 0:
                @pl.when(table(l, lost_out) == 1)
                def _():
                    send_pieces(slot, jnp.int32(lost), 1, True, False)
        return 0

    lax.fori_loop(0, 2, drain, 0)

    @pl.when(table(sec, has_slot[0]) == 1)
    def _():
        for j in range(N - 1):
            redistribute(j).wait_send()

    comes = table(sec, source)
    is_short = z < 2
    for part in (0, 1):
        for c in range(N):
            expected = (comes >= 0) & jnp.logical_not((comes == sec) & (me == c))
            if part:
                expected = expected & is_short

            @pl.when(expected)
            def _():
                pltpu.make_async_copy(orow.at[part, c], orow.at[part, c], o_recv.at[part, c]).wait()

    for part in (0, 1):
        has = (comes >= 0) & is_short if part else comes >= 0

        @pl.when(has)
        def _():
            for c in range(N):
                out_ref[part, :, c * BLK:(c + 1) * BLK] = orow[part, c].reshape(2, BLK).astype(jnp.bfloat16)

        @pl.when(jnp.logical_not(has))
        def _():
            out_ref[part] = jnp.zeros((2, N * BLK), jnp.bfloat16)


def relay(moved, counts, tokens, gains, w_in, w_out, b_in, b_out):
    bf, f32 = jnp.bfloat16, jnp.float32
    dma = pltpu.SemaphoreType.DMA
    anywhere = pl.BlockSpec(memory_space=pl.ANY)
    return pl.pallas_call(
        functools.partial(relay_kernel, moved),
        out_shape=jax.ShapeDtypeStruct((2, 2, N * BLK), bf),
        in_specs=[pl.BlockSpec(memory_space=pltpu.SMEM)] + [anywhere] * 6,
        out_specs=pl.BlockSpec(memory_space=pltpu.VMEM),
        scratch_shapes=[
            pltpu.VMEM((2, FULL, N * BLK), bf),
            pltpu.VMEM((4, N * BLK), bf),
            pltpu.VMEM((2, NZ, 2, UNITS, NXY * BLK), bf),
            pltpu.VMEM((2, N, UNITS, BLK), bf),
            pltpu.VMEM((2, NZ, NXY, ROWS, BLK), bf),
            pltpu.VMEM((2, N, ROWS, BLK), bf),
            pltpu.VMEM((2, N, ROWS, BLK), bf),
            pltpu.VMEM((2, ROWS, BLK), bf),
            pltpu.VMEM((2, ROWS, 1, BLK), f32),
            pltpu.VMEM((2, N, 2, 1, BLK), f32),
            pltpu.VMEM((ROWS, UNITS), f32),
            pltpu.VMEM((ROWS, UNITS), f32),
            pltpu.VMEM((ROWS, BLK), f32),
            dma((2,)),
            dma((2, NZ, 2)),
            dma((2, N)),
            dma((N,)),
            dma((2, N)),
            dma((2, N)),
            dma((2, N)),
            dma((2, NZ, NXY)),
            dma((2, 2, 2, N)),
            dma((2, N)),
        ],
        compiler_params=pltpu.CompilerParams(
            collective_id=PLANS.index(moved), has_side_effects=True, vmem_limit_bytes=60 * 1024 * 1024
        ),
    )(counts, tokens, gains, w_in, w_out, b_in, b_out)


def shards(tokens, norm_gain, w_in, w_out, backup_in, backup_out, layer_group, token_counts):
    sec = lax.axis_index("section")
    me = lax.axis_index(TENSOR)
    moved = [(layer_group[l] == l + 1).astype(jnp.int32) for l in range(3)]
    code = moved[0] * 4 + moved[1] * 2 + moved[2]
    codes = [p[0] * 4 + p[1] * 2 + p[2] for p in PLANS]
    plan = sum(jnp.where(code == c, k, 0) for k, c in enumerate(codes))
    rows = lax.switch(
        plan,
        [functools.partial(relay, p) for p in PLANS],
        token_counts, tokens, norm_gain, w_in[0], w_out[0], backup_in[0], backup_out[0],
    )
    kept = lax.dynamic_slice_in_dim(tokens, me * 2, 2, axis=1)
    full = jnp.where(token_counts[1] == FULL, 1, 0)
    batch = jnp.arange(2, dtype=jnp.int32)[:, None, None]
    computed = jnp.where(batch == full, rows[0][None], rows[1][None])
    untouched = ((moved[0] == 1) & (sec == 0)) | ((batch != full) & (me >= SHORT // 2))
    return jnp.where(untouched, kept, computed)[None]


def solution(mesh):
    finer = Mesh(mesh.devices.reshape(4, NZ, NX, NY), AXES)
    return jax.shard_map(
        shards,
        mesh=finer,
        in_specs=(
            P(),
            P(),
            P("section", None, TENSOR, None),
            P("section", TENSOR, None),
            P("section", None, TENSOR, None),
            P("section", None, TENSOR),
            P(),
            P(),
        ),
        out_specs=P("section", None, TENSOR, None),
        check_vma=False,
    )
```

```python
import functools

import jax
import jax.numpy as jnp
from jax import lax
from jax.experimental import pallas as pl
from jax.experimental.pallas import tpu as pltpu
from jax.sharding import Mesh
from jax.sharding import PartitionSpec as P

TENSOR = ("z", "xhi", "y")
AXES = ("section", "z", "xhi", "y")
MESH_ID = pl.DeviceIdType.MESH
NORM_EPS = 0.25
PLANS = ((1, 0, 0), (1, 1, 0), (1, 1, 1), (0, 1, 0), (0, 1, 1), (0, 0, 1))
NZ, NX, NY = 4, 2, 4
NXY = NX * NY
N = NZ * NXY
SEND_DZ = (2, 1, 3, 0)
TAKE_DZ = (0, 1, 3, 2)
XY = ((1, 2), (1, 1), (1, 3), (0, 2), (1, 0), (0, 1), (0, 3), (0, 0))
XY_BACK = [XY.index((-b % NX, -c % NY)) for b, c in XY]
FULL, SHORT = 64, 32
ROWS = FULL + SHORT
BLK = 128
UNITS = 448


def table(index, values):
    out = jnp.int32(values[-1])
    for k in range(len(values) - 2, -1, -1):
        if values[k] != values[-1]:
            out = jnp.where(index == k, jnp.int32(values[k]), out)
    return out


def relay_kernel(
    moved,
    counts, tokens, gains, w_in, w_out, b_in, b_out,
    out_ref,
    tok_v, gain_v, wg, wd, xbuf, ps, rs, xs, xpair, orow, kept, accg, accu, ssq, tot, prow, rrow, xrow, hid_v, hbuf,
    tok_sem, wg_sem, wd_sem, rd_send, rs_send, rs_recv, ag_send, ag_recv, o_send, o_recv, p_send, p_recv,
    h_send, h_recv, turn,
):
    m = tuple(moved) + (0,)
    runs = [l + m[l] for l in range(4)]
    reached = [sum(e <= g for e in runs) for g in range(4)]
    lost = moved.index(1)
    next_group = [runs[l + 1] if l < 3 else 0 for l in range(4)]
    next_slot = [1 - m[l + 1] if l < 3 else 0 for l in range(4)]
    own_out = [int(l < 3 and reached[runs[l]] == l + 1) for l in range(4)]
    lost_out = [int(lost > 0 and reached[lost] == l + 1) for l in range(4)]
    has_moved = [int(g > 0 and m[g - 1] == 1) for g in range(4)]
    has_own = [1 - m[g] for g in range(4)]
    source = [runs[r - 1] if r > 0 else -1 for r in reached]
    n_out = 2 if lost > 0 else 1
    gathers = m[0] == 1
    has_spread = [int(has_moved[g] == 1 and not (gathers and g == 1)) for g in range(4)]
    in_turn = m[1] == 1 and m[2] == 1

    sec = lax.axis_index("section")
    z, xh, y = (lax.axis_index(a) for a in TENSOR)
    xy = xh * NY + y
    me = z * NXY + xy
    zs = [lax.rem(z + d, NZ) for d in range(NZ)]
    xs_of = [lax.rem(xh + d, NX) for d in range(NX)]
    ys = [lax.rem(y + d, NY) for d in range(NY)]
    runs_moved = table(sec, has_moved) == 1
    runs_own = table(sec, has_own) == 1
    spreads = table(sec, has_spread) == 1

    def shifted(dz):
        return lax.rem(z + dz, NZ)

    def scope(name):
        return jax.named_scope(name)

    tok_copy = pltpu.make_async_copy(tokens, tok_v, tok_sem.at[0])
    gain_copy = pltpu.make_async_copy(gains, gain_v, tok_sem.at[1])
    tok_copy.start()
    gain_copy.start()

    def load_in(slot, src):
        def go(i, _):
            start = pl.multiple_of(shifted(table(i, TAKE_DZ)) * (NXY * BLK), NXY * BLK)
            for half in range(2):
                pltpu.make_async_copy(
                    src.at[half, :, pl.ds(start, NXY * BLK)], wg.at[slot, i, half], wg_sem.at[slot, i]
                ).start()
            return 0
        lax.fori_loop(0, NZ, go, 0)

    @pl.when(runs_moved)
    def _():
        load_in(0, b_in)

    if gathers:
        @pl.when(sec == 1)
        def _():
            def go(i, _):
                zz = shifted(table(i, TAKE_DZ))
                for k, (dx, dy) in enumerate(XY):
                    start = pl.multiple_of((zz * NXY + xs_of[dx] * NY + ys[dy]) * UNITS, UNITS)
                    pltpu.make_async_copy(b_out.at[pl.ds(start, UNITS), :], wd.at[0, i * NXY + k], wd_sem.at[0, i]).start()
                return 0
            lax.fori_loop(0, NZ, go, 0)

    @pl.when(runs_own)
    def _():
        load_in(1, w_in)

        def go(a, _):
            zz = shifted(table(a, SEND_DZ))
            for k, (dx, dy) in enumerate(XY):
                start = pl.multiple_of((zz * NXY + xs_of[dx] * NY + ys[dy]) * BLK, BLK)
                pltpu.make_async_copy(w_out.at[:, pl.ds(start, BLK)], wd.at[1, a * NXY + k], wd_sem.at[1, a]).start()
            return 0
        lax.fori_loop(0, NZ, go, 0)

    barrier = pltpu.get_barrier_semaphore()

    def greet(g, skip_self):
        for a in range(NZ):
            for k, (dx, dy) in enumerate(XY):
                if skip_self and a == NZ - 1 and k == NXY - 1:
                    continue
                pl.semaphore_signal(
                    barrier, inc=1, device_id=(g, zs[SEND_DZ[a]], xs_of[dx], ys[dy]), device_id_type=MESH_ID
                )

    with scope("greet"):
        greet(sec, True)

        def others(d, _):
            greet(lax.rem(sec + d, 4), False)
            return 0

        lax.fori_loop(1, 4, others, 0)

    def spread(a, k):
        dx, dy = XY[k]
        zz = zs[SEND_DZ[a]]
        start = pl.multiple_of((zz * NXY + xs_of[dx] * NY + ys[dy]) * UNITS, UNITS)
        back = (0, 2, 1, 3)[a]
        return pltpu.make_async_remote_copy(
            src_ref=b_out.at[pl.ds(start, UNITS), :], dst_ref=wd.at[0, back * NXY + XY_BACK[k]],
            send_sem=rd_send.at[0], recv_sem=wd_sem.at[0, back],
            device_id=(sec, zz, xs_of[dx], ys[dy]), device_id_type=MESH_ID,
        )

    def landed(ref, sem):
        pltpu.make_async_copy(ref, ref, sem).wait()

    def peers(go, to_self=None):
        def step(a, _):
            for k in range(NXY):
                if k < NXY - 1:
                    go(a, k)
                else:
                    pl.when(a < NZ - 1)(lambda: go(a, k))
                    if to_self is not None:
                        pl.when(a == NZ - 1)(lambda: to_self(a, k))
            return 0
        lax.fori_loop(0, NZ, step, 0)

    def meet():
        with scope("barrier"):
            pl.semaphore_wait(barrier, 4 * N - 1)

        @pl.when(spreads)
        def _():
            if in_turn:
                pl.when(sec == 3)(lambda: pl.semaphore_wait(turn, 1))
            with scope("redist"):
                start = pl.multiple_of(me * UNITS, UNITS)
                pltpu.make_async_copy(b_out.at[pl.ds(start, UNITS), :], wd.at[0, N - 1], wd_sem.at[0, NZ - 1]).start()
                for n in range(NXY):
                    for a in range(NZ):
                        k = (n + 2 * a) % NXY
                        if (a, k) != (NZ - 1, NXY - 1):
                            spread(a, k).start()

    def whole_down():
        for a in range(NZ):
            landed(wd.at[0, pl.ds(a * NXY, NXY)], wd_sem.at[0, a])
        if in_turn:
            @pl.when(sec == 2)
            def _():
                pl.semaphore_signal(turn, inc=1, device_id=(3, z, xh, y), device_id_type=MESH_ID)

    pl.when(sec != runs[0])(meet)

    full = jnp.where(counts[1] == FULL, 1, 0)
    short_count = jnp.where(full == 1, counts[0], counts[1])
    with scope("tokwait"):
        tok_copy.wait()
        gain_copy.wait()

    first_slot = 1 - m[0]

    @pl.when(sec == runs[0])
    def _():
        def go(i, _):
            zz = shifted(table(i, TAKE_DZ))
            for k in range(NXY):
                cols = pl.ds(pl.multiple_of((zz * NXY + k) * BLK, BLK), BLK)
                xbuf[first_slot, i * NXY + k, 0:FULL, :] = tok_v[full, :, cols]
                xbuf[first_slot, i * NXY + k, FULL:ROWS, :] = tok_v[1 - full, 0:SHORT, cols]
            return 0
        lax.fori_loop(0, NZ, go, 0)

    def find_kept():
        with scope("kept"):
            pick = lax.broadcasted_iota(jnp.int32, (8, FULL), 1) == me * 2 + lax.broadcasted_iota(jnp.int32, (8, FULL), 0)
            pick = jnp.where(pick, 1.0, 0.0).astype(jnp.bfloat16)
            for b in range(2):
                def go(c, _):
                    cols = pl.ds(pl.multiple_of(c * (NXY * BLK), NXY * BLK), NXY * BLK)
                    rows = jnp.dot(pick, tok_v[b, :, cols], preferred_element_type=jnp.float32)
                    kept[b, :, cols] = rows[0:2].astype(jnp.bfloat16)
                    return 0
                lax.fori_loop(0, NZ, go, 0)

    pl.when(sec != runs[0])(find_kept)

    row = lax.broadcasted_iota(jnp.int32, (ROWS, 1), 0)
    keep = jnp.where(row < FULL + short_count, 1.0, 0.0)

    def rs_copy(slot, a, k):
        dx, dy = XY[k]
        return pltpu.make_async_remote_copy(
            src_ref=ps.at[slot, a * NXY + k], dst_ref=rs.at[slot, (NZ - 1 - a) * NXY + XY_BACK[k]],
            send_sem=rs_send.at[slot], recv_sem=rs_recv.at[slot, NZ - 1 - a],
            device_id=(sec, shifted(table(a, SEND_DZ)), xs_of[dx], ys[dy]), device_id_type=MESH_ID,
        )

    def ag_copy(slot, to_group, to_slot, a, k):
        dx, dy = XY[k]
        return pltpu.make_async_remote_copy(
            src_ref=xs.at[slot], dst_ref=xbuf.at[to_slot, (NZ - 1 - a) * NXY + xy],
            send_sem=ag_send.at[slot], recv_sem=ag_recv.at[to_slot, NZ - 1 - a],
            device_id=(to_group, shifted(table(a, SEND_DZ)), xs_of[dx], ys[dy]), device_id_type=MESH_ID,
        )

    def piece(slot, which, to_group, part, a, k):
        dx, dy = XY[k]
        zz = shifted(table(a, SEND_DZ))
        first = zz * NXY + xs_of[dx] * NY + ys[dy] + (FULL // 2 if part else 0)
        return pltpu.make_async_remote_copy(
            src_ref=xpair.at[slot, first], dst_ref=orow.at[part, :, pl.ds(pl.multiple_of(me * BLK, BLK), BLK)],
            send_sem=o_send.at[slot, which, part], recv_sem=o_recv.at[part],
            device_id=(to_group, zz, xs_of[dx], ys[dy]), device_id_type=MESH_ID,
        )

    def pieces(slot, l):
        def each(which, _):
            to_group = jnp.where(which == 0, sec, lost)
            wanted = jnp.where(which == 0, table(l, own_out), table(l, lost_out)) == 1

            def go(a, k):
                piece(slot, which, to_group, 0, a, k).start()
                pl.when(shifted(table(a, SEND_DZ)) < NZ // 2)(lambda: piece(slot, which, to_group, 1, a, k).start())

            def to_self(a, k):
                pl.when(which == 1)(lambda: go(a, k))

                @pl.when(which == 0)
                def _():
                    cols = pl.ds(pl.multiple_of(me * BLK, BLK), BLK)
                    orow[0, :, cols] = xpair[slot, me]

                    @pl.when(z < NZ // 2)
                    def _():
                        orow[1, :, cols] = xpair[slot, FULL // 2 + me]

            pl.when(wanted)(lambda: peers(go, to_self))
            return 0

        lax.fori_loop(0, n_out, each, 0)

    def pieces_out(slot, l):
        half = N // 2
        for which in range(n_out):
            @pl.when(table(l, lost_out if which else own_out) == 1)
            def _():
                if which:
                    landed(xpair.at[slot, pl.ds(0, N)], o_send.at[slot, which, 0])
                    landed(xpair.at[slot, pl.ds(0, half)], o_send.at[slot, which, 1])
                else:
                    landed(xpair.at[slot, pl.ds(0, N - 1)], o_send.at[slot, which, 0])
                    pl.when(z < NZ // 2)(lambda: landed(xpair.at[slot, pl.ds(0, half - 1)], o_send.at[slot, which, 1]))
                    pl.when(z >= NZ // 2)(lambda: landed(xpair.at[slot, pl.ds(0, half)], o_send.at[slot, which, 1]))

    def row_copy(part, a, k):
        dx, dy = XY[k]
        zz = shifted(table(a, SEND_DZ))
        first = zz * NXY + xs_of[dx] * NY + ys[dy] + (FULL // 2 if part else 0)
        return pltpu.make_async_remote_copy(
            src_ref=prow.at[first], dst_ref=rrow.at[part, (NZ - 1 - a) * NXY + XY_BACK[k]],
            send_sem=p_send.at[part], recv_sem=p_recv.at[part, NZ - 1 - a],
            device_id=(sec, zz, xs_of[dx], ys[dy]), device_id_type=MESH_ID,
        )

    def finish_rows():
        with scope("rowsend"):
            def go(a, k):
                row_copy(0, a, k).start()
                pl.when(shifted(table(a, SEND_DZ)) < NZ // 2)(lambda: row_copy(1, a, k).start())

            peers(go)
        with scope("rowpick"):
            r = lax.broadcasted_iota(jnp.int32, (8, ROWS), 0)
            c = lax.broadcasted_iota(jnp.int32, (8, ROWS), 1)
            pick = jnp.where(c == me * 2 + jnp.where(r < 2, r, r - 2 + FULL), 1.0, 0.0)
            pick = jnp.where((r < 2) | (z < NZ // 2), pick, 0.0).astype(jnp.bfloat16)

            def fetch(i, _):
                cols = pl.ds(pl.multiple_of(shifted(table(i, TAKE_DZ)) * (NXY * BLK), NXY * BLK), NXY * BLK)
                x = jnp.concatenate([xbuf[1, i * NXY + k] for k in range(NXY)], axis=1)
                xrow[:, cols] = jnp.dot(pick, x, preferred_element_type=jnp.float32)
                return 0

            lax.fori_loop(0, NZ, fetch, 0)
            rrow[0, N // NZ - 1] = prow[me]

            @pl.when(z < NZ // 2)
            def _():
                rrow[1, N // NZ - 1] = prow[FULL // 2 + me]

        def total_of(part):
            def take(i, total):
                pl.when(i == 0)(lambda: landed(rrow.at[part, pl.ds(0, NXY - 1)], p_recv.at[part, 0]))
                pl.when(i > 0)(lambda: landed(rrow.at[part, pl.ds(i * NXY, NXY)], p_recv.at[part, i]))
                for k in range(NXY):
                    total += rrow[part, i * NXY + k].astype(jnp.float32)
                return total
            return lax.fori_loop(0, NZ, take, jnp.zeros((2, N * BLK), jnp.float32))

        with scope("rowsum"):
            orow[0] = (xrow[0:2, :] + total_of(0)).astype(jnp.bfloat16)

            @pl.when(z < NZ // 2)
            def _():
                r = lax.broadcasted_iota(jnp.int32, (2, 1), 0) + me * 2
                orow[1] = (xrow[2:4, :] + jnp.where(r < short_count, 1.0, 0.0) * total_of(1)).astype(jnp.bfloat16)

    def h_copy(a, k):
        dx, dy = XY[k]
        return pltpu.make_async_remote_copy(
            src_ref=hid_v, dst_ref=hbuf.at[(NZ - 1 - a) * NXY + XY_BACK[k]],
            send_sem=h_send.at[0], recv_sem=h_recv.at[NZ - 1 - a],
            device_id=(sec, shifted(table(a, SEND_DZ)), xs_of[dx], ys[dy]), device_id_type=MESH_ID,
        )

    def gathered_down(hidden):
        hid_v[...] = hidden
        hbuf[NXY - 1] = hidden
        with scope("hsend"):
            peers(lambda a, k: h_copy(a, k).start())
        tot[...] = jnp.zeros_like(tot)

        def take(i, _):
            with scope("hdown"):
                landed(wd.at[0, pl.ds(i * NXY, NXY)], wd_sem.at[0, i])
                pl.when(i == 0)(lambda: landed(hbuf.at[pl.ds(0, NXY - 1)], h_recv.at[0]))
                pl.when(i > 0)(lambda: landed(hbuf.at[pl.ds(i * NXY, NXY)], h_recv.at[i]))
                total = tot[...]
                for k in range(NXY):
                    block = jnp.dot(hbuf[i * NXY + k], wd[0, i * NXY + k], preferred_element_type=jnp.float32)
                    total += block.astype(jnp.bfloat16).astype(jnp.float32)
                tot[...] = total
            return 0

        lax.fori_loop(0, NZ, take, 0)

    def gate_up(slot, l, i):
        zz = shifted(table(i, TAKE_DZ))

        @pl.when(l > 0)
        def _():
            short = (i == 0) & (slot == 1) & runs_moved

            @pl.when(short)
            def _():
                landed(xbuf.at[slot, pl.ds(0, NXY - 1)], ag_recv.at[slot, 0])

            @pl.when(jnp.logical_not(short))
            def _():
                landed(xbuf.at[slot, pl.ds(i * NXY, NXY)], ag_recv.at[slot, i])

        landed(wg.at[slot, i], wg_sem.at[slot, i])
        cols = pl.ds(pl.multiple_of(zz * (NXY * BLK), NXY * BLK), NXY * BLK)
        which = lax.broadcasted_iota(jnp.int32, (4, 1), 0)
        gain = jnp.sum(jnp.where(which == l, gain_v[:, cols].astype(jnp.float32), 0.0), axis=0, keepdims=True)
        squares = ssq[...]
        parts = []
        for k in range(NXY):
            xf = xbuf[slot, i * NXY + k].astype(jnp.float32)
            squares += xf * xf
            parts.append((xf * gain[:, k * BLK:(k + 1) * BLK]).astype(jnp.bfloat16))
        ssq[...] = squares
        lhs = jnp.concatenate(parts, axis=1)
        dims = (((1,), (1,)), ((), ()))
        accg[...] += lax.dot_general(lhs, wg[slot, i, 0], dims, preferred_element_type=jnp.float32)
        accu[...] += lax.dot_general(lhs, wg[slot, i, 1], dims, preferred_element_type=jnp.float32)

    def layer(slot, _):
        l = sec - 1 + slot
        to_group = table(l, next_group)
        to_slot = table(l, next_slot)
        stays = to_group == sec

        @pl.when(jnp.where(slot == 0, runs_moved, runs_own))
        def _():
            accg[...] = jnp.zeros_like(accg)
            accu[...] = jnp.zeros_like(accu)
            ssq[...] = jnp.zeros_like(ssq)
            if in_turn and gathers:
                pl.when(spreads & (slot == 0))(whole_down)

            def step(i, _):
                with scope("gu"):
                    gate_up(slot, l, i)
                return 0

            lax.fori_loop(0, NZ, step, 0)
            with scope("hid"):
                mean = jnp.sum(ssq[...], axis=1, keepdims=True) * (1.0 / (N * BLK))
                scale = lax.rsqrt(mean + NORM_EPS)
                gate = accg[...] * scale
                hidden = (gate / (1.0 + jnp.exp(-gate)) * (accu[...] * scale)).astype(jnp.bfloat16)
            pl.when(l == 0)(meet)
            if not (in_turn and gathers):
                with scope("wdwait"):
                    pl.when(spreads & (slot == 0))(whole_down)

            def down(a, _):
                with scope("down"):
                    pl.when(slot == 1)(lambda: landed(wd.at[1, pl.ds(a * NXY, NXY)], wd_sem.at[1, a]))
                    w = jnp.concatenate([wd[slot, a * NXY + k] for k in range(NXY)], axis=1)
                    part = jnp.dot(hidden, w, preferred_element_type=jnp.float32).astype(jnp.bfloat16)

                    @pl.when(l < 3)
                    def _():
                        for k in range(NXY):
                            ps[slot, a * NXY + k] = part[:, k * BLK:(k + 1) * BLK]
                        for k in range(NXY - 1):
                            rs_copy(slot, a, k).start()
                        pl.when(a < NZ - 1)(lambda: rs_copy(slot, a, NXY - 1).start())

                    @pl.when(l == 3)
                    def _():
                        zz = shifted(table(a, SEND_DZ))
                        for k, (dx, dy) in enumerate(XY):
                            cols = pl.ds(pl.multiple_of((zz * NXY + xs_of[dx] * NY + ys[dy]) * BLK, BLK), BLK)
                            prow[:, :, cols] = part[:, k * BLK:(k + 1) * BLK].reshape(ROWS // 2, 2, BLK)
                return 0

            def reduced_down():
                lax.fori_loop(0, NZ, down, 0)

                @pl.when(l < 3)
                def _():
                    rs[slot, NXY - 1] = ps[slot, N - 1]

                    def take(i, total):
                        pl.when(i == 0)(lambda: landed(rs.at[slot, pl.ds(0, NXY - 1)], rs_recv.at[slot, 0]))
                        pl.when(i > 0)(lambda: landed(rs.at[slot, pl.ds(i * NXY, NXY)], rs_recv.at[slot, i]))
                        for k in range(NXY):
                            total += rs[slot, i * NXY + k].astype(jnp.float32)
                        return total

                    with scope("sum"):
                        tot[...] = lax.fori_loop(0, NZ, take, jnp.zeros((ROWS, BLK), jnp.float32))

            if gathers:
                pl.when(l == 0)(lambda: gathered_down(hidden))
                pl.when(l > 0)(reduced_down)
            else:
                reduced_down()

            @pl.when(l < 3)
            def _():
                new = (xbuf[slot, xy].astype(jnp.float32) + keep * tot[...]).astype(jnp.bfloat16)
                xs[slot] = new
                with scope("ag"):
                    def at_home(a, k):
                        @pl.when(stays)
                        def _():
                            xbuf[1, xy] = new

                        pl.when(jnp.logical_not(stays))(lambda: ag_copy(slot, to_group, to_slot, a, k).start())

                    peers(lambda a, k: ag_copy(slot, to_group, to_slot, a, k).start(), at_home)
                xpair[slot] = new.reshape(ROWS // 2, 2, BLK)
                with scope("pieces"):
                    pieces(slot, l)

            pl.when(l == 3)(finish_rows)
        return 0

    lax.fori_loop(0, 2, layer, 0)
    pl.when(sec == runs[0])(find_kept)

    comes = table(sec, source)
    with scope("rows"):
        for part in (0, 1):
            def wait_rows(count):
                landed(orow.at[part, :, pl.ds(0, count * BLK)], o_recv.at[part])

            here = (comes >= 0) & (sec < 3)
            if part:
                here = here & (z < NZ // 2)
            pl.when(here & (comes == sec))(lambda: wait_rows(N - 1))
            pl.when(here & (comes != sec))(lambda: wait_rows(N))

    @pl.when(comes < 0)
    def _():
        orow[0] = kept[0]

    @pl.when((comes < 0) | (z >= NZ // 2))
    def _():
        orow[1] = kept[1]

    with scope("assemble"):
        touched_full = comes >= 0
        touched_short = (comes >= 0) & (z < NZ // 2)
        for b in range(2):
            computed = jnp.where(full == b, orow[0].astype(jnp.float32), orow[1].astype(jnp.float32))
            use = jnp.where(full == b, jnp.where(touched_full, 1, 0), jnp.where(touched_short, 1, 0)) == 1
            out_ref[b] = jnp.where(use, computed, kept[b].astype(jnp.float32)).astype(jnp.bfloat16)

    def drain(slot, _):
        l = sec - 1 + slot
        to_group = table(l, next_group)
        to_slot = table(l, next_slot)
        stays = to_group == sec

        @pl.when(jnp.where(slot == 0, runs_moved, runs_own))
        def _():
            if gathers:
                pl.when(l == 0)(lambda: landed(hbuf.at[pl.ds(0, N - 1)], h_send.at[0]))

            @pl.when(l < 3)
            def _():
                by_sums = l > 0 if gathers else l >= 0
                pl.when(by_sums)(lambda: landed(ps.at[slot, pl.ds(0, N - 1)], rs_send.at[slot]))
                pl.when(stays)(lambda: landed(ps.at[slot, pl.ds(0, N - 1)], ag_send.at[slot]))
                pl.when(jnp.logical_not(stays))(lambda: landed(ps.at[slot], ag_send.at[slot]))
                pieces_out(slot, l)

            @pl.when(l == 3)
            def _():
                landed(prow.at[pl.ds(0, N - 1)], p_send.at[0])
                pl.when(z < NZ // 2)(lambda: landed(prow.at[pl.ds(0, N // 2 - 1)], p_send.at[1]))
                pl.when(z >= NZ // 2)(lambda: landed(prow.at[pl.ds(0, N // 2)], p_send.at[1]))
        return 0

    with scope("drain"):
        lax.fori_loop(0, 2, drain, 0)
        pl.when(spreads)(lambda: landed(wd.at[0, pl.ds(0, N - 1)], rd_send.at[0]))


def relay(moved, counts, tokens, gains, w_in, w_out, b_in, b_out):
    bf, f32 = jnp.bfloat16, jnp.float32
    dma = pltpu.SemaphoreType.DMA
    anywhere = pl.BlockSpec(memory_space=pl.ANY)
    return pl.pallas_call(
        functools.partial(relay_kernel, moved),
        out_shape=jax.ShapeDtypeStruct((2, 2, N * BLK), bf),
        in_specs=[pl.BlockSpec(memory_space=pltpu.SMEM)] + [anywhere] * 6,
        out_specs=pl.BlockSpec(memory_space=pltpu.VMEM),
        scratch_shapes=[
            pltpu.VMEM((2, FULL, N * BLK), bf),
            pltpu.VMEM((4, N * BLK), bf),
            pltpu.VMEM((2, NZ, 2, UNITS, NXY * BLK), bf),
            pltpu.VMEM((2, N, UNITS, BLK), bf),
            pltpu.VMEM((2, N, ROWS, BLK), bf),
            pltpu.VMEM((2, N, ROWS, BLK), bf),
            pltpu.VMEM((2, N, ROWS, BLK), bf),
            pltpu.VMEM((2, ROWS, BLK), bf),
            pltpu.VMEM((2, ROWS // 2, 2, BLK), bf),
            pltpu.VMEM((2, 2, N * BLK), bf),
            pltpu.VMEM((2, 2, N * BLK), bf),
            pltpu.VMEM((ROWS, UNITS), f32),
            pltpu.VMEM((ROWS, UNITS), f32),
            pltpu.VMEM((ROWS, BLK), f32),
            pltpu.VMEM((ROWS, BLK), f32),
            pltpu.VMEM((ROWS // 2, 2, N * BLK), bf),
            pltpu.VMEM((2, N, 2, N * BLK), bf),
            pltpu.VMEM((8, N * BLK), f32),
            pltpu.VMEM((ROWS, UNITS), bf),
            pltpu.VMEM((N, ROWS, UNITS), bf),
            dma((2,)),
            dma((2, NZ)),
            dma((2, NZ)),
            dma((1,)),
            dma((2,)),
            dma((2, NZ)),
            dma((2,)),
            dma((2, NZ)),
            dma((2, 2, 2)),
            dma((2,)),
            dma((2,)),
            dma((2, NZ)),
            dma((1,)),
            dma((NZ,)),
            pltpu.SemaphoreType.REGULAR,
        ],
        compiler_params=pltpu.CompilerParams(
            collective_id=PLANS.index(moved), has_side_effects=True, vmem_limit_bytes=60 * 1024 * 1024
        ),
    )(counts, tokens, gains, w_in, w_out, b_in, b_out)


def shards(tokens, norm_gain, w_in, w_out, backup_in, backup_out, layer_group, token_counts):
    code = (layer_group[0] == 1) * 4 + (layer_group[1] == 2) * 2 + (layer_group[2] == 3)
    codes = [p[0] * 4 + p[1] * 2 + p[2] for p in PLANS]
    plan = sum(jnp.where(code == c, k, 0) for k, c in enumerate(codes))
    rows = lax.switch(
        plan,
        [functools.partial(relay, p) for p in PLANS],
        token_counts, tokens, norm_gain, w_in[0], w_out[0], backup_in[0], backup_out[0],
    )
    return rows[None]


def solution(mesh):
    finer = Mesh(mesh.devices.reshape(4, NZ, NX, NY), AXES)
    return jax.shard_map(
        shards,
        mesh=finer,
        in_specs=(
            P(),
            P(),
            P("section", None, TENSOR, None),
            P("section", TENSOR, None),
            P("section", None, TENSOR, None),
            P("section", None, TENSOR),
            P(),
            P(),
        ),
        out_specs=P("section", None, TENSOR, None),
        check_vma=False,
    )
```

```python
import functools

import jax
import jax.numpy as jnp
from jax import lax
from jax.experimental import pallas as pl
from jax.experimental.pallas import tpu as pltpu
from jax.sharding import Mesh
from jax.sharding import PartitionSpec as P

TENSOR = ("z", "xhi", "y")
AXES = ("section", "z", "xhi", "y")
MESH_ID = pl.DeviceIdType.MESH
NORM_EPS = 0.25
HOW = ("--R", "H--", "-H-", "-HH", "HR-", "HRH")
PLANS = ((0, 0, 1), (1, 0, 0), (0, 1, 0), (0, 1, 1), (1, 1, 0), (1, 1, 1))
PLAN_WEIGHTS = (2, 3, 1, 0)
NZ, NX, NY = 4, 2, 4
NXY = NX * NY
N = NZ * NXY
SEND_DZ = (2, 1, 3, 0)
TAKE_DZ = (0, 1, 3, 2)
XY = ((1, 2), (1, 1), (1, 3), (0, 2), (1, 0), (0, 1), (0, 3), (0, 0))
ZX = ((2, 1), (1, 1), (3, 1), (2, 0), (0, 1), (1, 0), (3, 0))
ZX_BACK = [ZX.index((-a % NZ, -b % NX)) for a, b in ZX]
XY_BACK = [XY.index((-b % NX, -c % NY)) for b, c in XY]
FULL, SHORT = 64, 32
ROWS = FULL + SHORT
BLK = 128
UNITS = 448


def table(index, values):
    out = jnp.int32(values[-1])
    for k in range(len(values) - 2, -1, -1):
        if values[k] != values[-1]:
            out = jnp.where(index == k, jnp.int32(values[k]), out)
    return out


def relay_kernel(
    moved,
    counts, tokens, gains, w_in, w_out, b_in, b_out,
    out_ref,
    tok_v, gain_v, wg, wgt, wd, xbuf, ps, rs, xs, xpair, orow, kept, accg, accu, ssq, tot, prow, rrow, xrow, hbuf,
    tok_sem, wg_sem, wd_sem, rd_send, rs_send, rs_recv, ag_send, ag_recv, o_send, o_recv, p_send, p_recv,
    h_send, h1_recv, h2_recv,
):
    m = tuple(moved) + (0,)
    runs = [l + m[l] for l in range(4)]
    reached = [sum(e <= g for e in runs) for g in range(4)]
    lost = moved.index(1)
    next_group = [runs[l + 1] if l < 3 else 0 for l in range(4)]
    next_slot = [1 - m[l + 1] if l < 3 else 0 for l in range(4)]
    own_out = [int(l < 3 and reached[runs[l]] == l + 1) for l in range(4)]
    lost_out = [int(lost > 0 and reached[lost] == l + 1) for l in range(4)]
    has_moved = [int(g > 0 and m[g - 1] == 1) for g in range(4)]
    has_own = [1 - m[g] for g in range(4)]
    source = [runs[r - 1] if r > 0 else -1 for r in reached]
    n_out = 2 if lost > 0 else 1
    how = HOW[PLANS.index(moved)]
    has_gather = [int(g > 0 and how[g - 1] == "H") for g in range(4)]
    has_spread = [int(g > 0 and how[g - 1] == "R") for g in range(4)]
    any_gather, any_spread = sum(has_gather) > 0, sum(has_spread) > 0

    sec = lax.axis_index("section")
    z, xh, y = (lax.axis_index(a) for a in TENSOR)
    xy = xh * NY + y
    me = z * NXY + xy
    zs = [lax.rem(z + d, NZ) for d in range(NZ)]
    xs_of = [lax.rem(xh + d, NX) for d in range(NX)]
    ys = [lax.rem(y + d, NY) for d in range(NY)]
    runs_moved = table(sec, has_moved) == 1
    runs_own = table(sec, has_own) == 1
    spreads = table(sec, has_spread) == 1
    gathers = table(sec, has_gather) == 1

    def shifted(dz):
        return lax.rem(z + dz, NZ)

    def scope(name):
        return jax.named_scope(name)

    tok_copy = pltpu.make_async_copy(tokens, tok_v, tok_sem.at[0])
    gain_copy = pltpu.make_async_copy(gains, gain_v, tok_sem.at[1])
    tok_copy.start()
    gain_copy.start()

    def load_in(slot, src):
        def go(n, _):
            i = NZ - 1 - n
            start = pl.multiple_of(shifted(table(i, TAKE_DZ)) * (NXY * BLK), NXY * BLK)
            for half in range(2):
                pltpu.make_async_copy(
                    src.at[half, :, pl.ds(start, NXY * BLK)], wg.at[slot, i, half], wg_sem.at[slot, i]
                ).start()
            return 0
        lax.fori_loop(0, NZ, go, 0)

    @pl.when(runs_moved)
    def _():
        load_in(0, b_in)

    if any_gather:
        @pl.when(gathers)
        def _():
            def go(i, _):
                for k in range(NXY):
                    block = i * NXY + k
                    start = pl.multiple_of(block * UNITS, UNITS)
                    pltpu.make_async_copy(b_out.at[pl.ds(start, UNITS), :], wd.at[0, block], wd_sem.at[0, i]).start()
                return 0
            lax.fori_loop(0, NZ, go, 0)

    @pl.when(runs_own)
    def _():
        load_in(1, w_in)

        def go(a, _):
            zz = shifted(table(a, SEND_DZ))
            for k, (dx, dy) in enumerate(XY):
                start = pl.multiple_of((zz * NXY + xs_of[dx] * NY + ys[dy]) * BLK, BLK)
                pltpu.make_async_copy(w_out.at[:, pl.ds(start, BLK)], wd.at[1, a * NXY + k], wd_sem.at[1, a]).start()
            return 0
        lax.fori_loop(0, NZ, go, 0)

    barrier = pltpu.get_barrier_semaphore()

    def greet(g, skip_self):
        for a in range(NZ):
            for k, (dx, dy) in enumerate(XY):
                if skip_self and a == NZ - 1 and k == NXY - 1:
                    continue
                pl.semaphore_signal(
                    barrier, inc=1, device_id=(g, zs[SEND_DZ[a]], xs_of[dx], ys[dy]), device_id_type=MESH_ID
                )

    with scope("greet"):
        greet(sec, True)

        def others(d, _):
            greet(lax.rem(sec + d, 4), False)
            return 0

        lax.fori_loop(1, 4, others, 0)

    def spread(a, k):
        dx, dy = XY[k]
        zz = zs[SEND_DZ[a]]
        start = pl.multiple_of((zz * NXY + xs_of[dx] * NY + ys[dy]) * UNITS, UNITS)
        back = (0, 2, 1, 3)[a]
        return pltpu.make_async_remote_copy(
            src_ref=b_out.at[pl.ds(start, UNITS), :], dst_ref=wd.at[0, back * NXY + XY_BACK[k]],
            send_sem=rd_send.at[0], recv_sem=wd_sem.at[0, back],
            device_id=(sec, zz, xs_of[dx], ys[dy]), device_id_type=MESH_ID,
        )

    def landed(ref, sem):
        pltpu.make_async_copy(ref, ref, sem).wait()

    def peers(go, to_self=None):
        def step(a, _):
            for k in range(NXY):
                if k < NXY - 1:
                    go(a, k)
                else:
                    pl.when(a < NZ - 1)(lambda: go(a, k))
                    if to_self is not None:
                        pl.when(a == NZ - 1)(lambda: to_self(a, k))
            return 0
        lax.fori_loop(0, NZ, step, 0)

    def meet():
        with scope("barrier"):
            pl.semaphore_wait(barrier, 4 * N - 1)

        if any_spread:
            @pl.when(spreads)
            def _():
                with scope("redist"):
                    start = pl.multiple_of(me * UNITS, UNITS)
                    pltpu.make_async_copy(b_out.at[pl.ds(start, UNITS), :], wd.at[0, N - 1], wd_sem.at[0, NZ - 1]).start()
                    for n in range(NXY):
                        for a in range(NZ):
                            k = (n + 2 * a) % NXY
                            if (a, k) != (NZ - 1, NXY - 1):
                                spread(a, k).start()

    pl.when(sec != runs[0])(meet)

    full = jnp.where(counts[1] == FULL, 1, 0)
    short_count = jnp.where(full == 1, counts[0], counts[1])
    with scope("tokwait"):
        tok_copy.wait()
        gain_copy.wait()

    first_slot = 1 - m[0]

    @pl.when(sec == runs[0])
    def _():
        def go(i, _):
            zz = shifted(table(i, TAKE_DZ))
            for k in range(NXY):
                cols = pl.ds(pl.multiple_of((zz * NXY + k) * BLK, BLK), BLK)
                xbuf[first_slot, i * NXY + k, 0:FULL, :] = tok_v[full, :, cols]
                xbuf[first_slot, i * NXY + k, FULL:ROWS, :] = tok_v[1 - full, 0:SHORT, cols]
            return 0
        lax.fori_loop(0, NZ, go, 0)

    def find_kept():
        with scope("kept"):
            pick = lax.broadcasted_iota(jnp.int32, (8, FULL), 1) == me * 2 + lax.broadcasted_iota(jnp.int32, (8, FULL), 0)
            pick = jnp.where(pick, 1.0, 0.0).astype(jnp.bfloat16)
            for b in range(2):
                def go(c, _):
                    cols = pl.ds(pl.multiple_of(c * (NXY * BLK), NXY * BLK), NXY * BLK)
                    rows = jnp.dot(pick, tok_v[b, :, cols], preferred_element_type=jnp.float32)
                    kept[b, :, cols] = rows[0:2].astype(jnp.bfloat16)
                    return 0
                lax.fori_loop(0, NZ, go, 0)

    pl.when(sec != runs[0])(find_kept)

    turns = sec != runs[0]

    def turn(n, _):
        slot, half = n // (2 * NZ), lax.rem(n, 2)
        i = NZ - 1 - lax.rem(n, 2 * NZ) // 2

        @pl.when(jnp.where(slot == 0, runs_moved, runs_own))
        def _():
            pl.when(half == 0)(lambda: landed(wg.at[slot, i], wg_sem.at[slot, i]))
            with scope("turn"):
                wgt[slot, i, half] = wg[slot, i, half].T
        return 0

    @pl.when(turns)
    def _():
        lax.fori_loop(0, 4 * NZ, turn, 0)

    row = lax.broadcasted_iota(jnp.int32, (ROWS, 1), 0)
    keep = jnp.where(row < FULL + short_count, 1.0, 0.0)

    def rs_copy(slot, a, k):
        dx, dy = XY[k]
        return pltpu.make_async_remote_copy(
            src_ref=ps.at[slot, a * NXY + k], dst_ref=rs.at[slot, (NZ - 1 - a) * NXY + XY_BACK[k]],
            send_sem=rs_send.at[slot], recv_sem=rs_recv.at[slot, NZ - 1 - a],
            device_id=(sec, shifted(table(a, SEND_DZ)), xs_of[dx], ys[dy]), device_id_type=MESH_ID,
        )

    def ag_copy(slot, to_group, to_slot, a, k):
        dx, dy = XY[k]
        return pltpu.make_async_remote_copy(
            src_ref=xs.at[slot], dst_ref=xbuf.at[to_slot, (NZ - 1 - a) * NXY + xy],
            send_sem=ag_send.at[slot], recv_sem=ag_recv.at[to_slot, NZ - 1 - a],
            device_id=(to_group, shifted(table(a, SEND_DZ)), xs_of[dx], ys[dy]), device_id_type=MESH_ID,
        )

    def piece(slot, which, to_group, part, a, k):
        dx, dy = XY[k]
        zz = shifted(table(a, SEND_DZ))
        first = zz * NXY + xs_of[dx] * NY + ys[dy] + (FULL // 2 if part else 0)
        return pltpu.make_async_remote_copy(
            src_ref=xpair.at[slot, first], dst_ref=orow.at[part, :, pl.ds(pl.multiple_of(me * BLK, BLK), BLK)],
            send_sem=o_send.at[slot, which, part], recv_sem=o_recv.at[part],
            device_id=(to_group, zz, xs_of[dx], ys[dy]), device_id_type=MESH_ID,
        )

    def pieces(slot, l):
        def each(which, _):
            to_group = jnp.where(which == 0, sec, lost)
            wanted = jnp.where(which == 0, table(l, own_out), table(l, lost_out)) == 1

            def go(a, k):
                piece(slot, which, to_group, 0, a, k).start()
                pl.when(shifted(table(a, SEND_DZ)) < NZ // 2)(lambda: piece(slot, which, to_group, 1, a, k).start())

            def to_self(a, k):
                pl.when(which == 1)(lambda: go(a, k))

                @pl.when(which == 0)
                def _():
                    cols = pl.ds(pl.multiple_of(me * BLK, BLK), BLK)
                    orow[0, :, cols] = xpair[slot, me]

                    @pl.when(z < NZ // 2)
                    def _():
                        orow[1, :, cols] = xpair[slot, FULL // 2 + me]

            pl.when(wanted)(lambda: peers(go, to_self))
            return 0

        lax.fori_loop(0, n_out, each, 0)

    def pieces_out(slot, l):
        half = N // 2
        for which in range(n_out):
            @pl.when(table(l, lost_out if which else own_out) == 1)
            def _():
                if which:
                    landed(xpair.at[slot, pl.ds(0, N)], o_send.at[slot, which, 0])
                    landed(xpair.at[slot, pl.ds(0, half)], o_send.at[slot, which, 1])
                else:
                    landed(xpair.at[slot, pl.ds(0, N - 1)], o_send.at[slot, which, 0])
                    pl.when(z < NZ // 2)(lambda: landed(xpair.at[slot, pl.ds(0, half - 1)], o_send.at[slot, which, 1]))
                    pl.when(z >= NZ // 2)(lambda: landed(xpair.at[slot, pl.ds(0, half)], o_send.at[slot, which, 1]))

    def row_copy(part, a, k):
        dx, dy = XY[k]
        zz = shifted(table(a, SEND_DZ))
        first = zz * NXY + xs_of[dx] * NY + ys[dy] + (FULL // 2 if part else 0)
        return pltpu.make_async_remote_copy(
            src_ref=prow.at[first], dst_ref=rrow.at[part, (NZ - 1 - a) * NXY + XY_BACK[k]],
            send_sem=p_send.at[part], recv_sem=p_recv.at[part, NZ - 1 - a],
            device_id=(sec, zz, xs_of[dx], ys[dy]), device_id_type=MESH_ID,
        )

    def finish_rows():
        with scope("rowsend"):
            def go(a, k):
                row_copy(0, a, k).start()
                pl.when(shifted(table(a, SEND_DZ)) < NZ // 2)(lambda: row_copy(1, a, k).start())

            peers(go)
        with scope("rowpick"):
            r = lax.broadcasted_iota(jnp.int32, (8, ROWS), 0)
            c = lax.broadcasted_iota(jnp.int32, (8, ROWS), 1)
            pick = jnp.where(c == me * 2 + jnp.where(r < 2, r, r - 2 + FULL), 1.0, 0.0)
            pick = jnp.where((r < 2) | (z < NZ // 2), pick, 0.0).astype(jnp.bfloat16)

            def fetch(i, _):
                cols = pl.ds(pl.multiple_of(shifted(table(i, TAKE_DZ)) * (NXY * BLK), NXY * BLK), NXY * BLK)
                x = jnp.concatenate([xbuf[1, i * NXY + k] for k in range(NXY)], axis=1)
                xrow[:, cols] = jnp.dot(pick, x, preferred_element_type=jnp.float32)
                return 0

            lax.fori_loop(0, NZ, fetch, 0)
            rrow[0, N // NZ - 1] = prow[me]

            @pl.when(z < NZ // 2)
            def _():
                rrow[1, N // NZ - 1] = prow[FULL // 2 + me]

        def total_of(part):
            def take(i, total):
                pl.when(i == 0)(lambda: landed(rrow.at[part, pl.ds(0, NXY - 1)], p_recv.at[part, 0]))
                pl.when(i > 0)(lambda: landed(rrow.at[part, pl.ds(i * NXY, NXY)], p_recv.at[part, i]))
                for k in range(NXY):
                    total += rrow[part, i * NXY + k].astype(jnp.float32)
                return total
            return lax.fori_loop(0, NZ, take, jnp.zeros((2, N * BLK), jnp.float32))

        with scope("rowsum"):
            orow[0] = (xrow[0:2, :] + total_of(0)).astype(jnp.bfloat16)

            @pl.when(z < NZ // 2)
            def _():
                r = lax.broadcasted_iota(jnp.int32, (2, 1), 0) + me * 2
                orow[1] = (xrow[2:4, :] + jnp.where(r < short_count, 1.0, 0.0) * total_of(1)).astype(jnp.bfloat16)

    def half_block(half, src, to, recv):
        return pltpu.make_async_remote_copy(
            src_ref=hbuf.at[src, half], dst_ref=hbuf.at[src, half], send_sem=h_send.at[0], recv_sem=recv,
            device_id=(sec, *to), device_id_type=MESH_ID,
        )

    def along_z(src):
        for d in (2, 1, 3):
            half_block(0, src, (zs[d], xh, y), h2_recv.at[0, (-d) % NZ]).start()

    def along_y(src):
        for d in (2, 1, 3):
            half_block(1, src, (z, xh, ys[d]), h2_recv.at[1, (-d) % NY]).start()

    def gathered_down(hidden):
        hbuf[me] = hidden.reshape(2, ROWS // 2, UNITS)
        with scope("hsend"):
            for k in range(NXY - 1):
                dx, dy = XY[k]
                half_block(0, me, (z, xs_of[dx], ys[dy]), h1_recv.at[0, XY_BACK[k]]).start()
                dz, dx = ZX[k]
                half_block(1, me, (zs[dz], xs_of[dx], y), h1_recv.at[1, ZX_BACK[k]]).start()
            along_z(me)
            along_y(me)
        with scope("hforward"):
            for k in range(NXY - 2, -1, -1):
                dx, dy = XY[k]
                src = z * NXY + xs_of[dx] * NY + ys[dy]
                landed(hbuf.at[src, 0], h1_recv.at[0, k])
                along_z(src)
                dz, dx = ZX[k]
                src = zs[dz] * NXY + xs_of[dx] * NY + y
                landed(hbuf.at[src, 1], h1_recv.at[1, k])
                along_y(src)
        with scope("hwait"):
            for half in range(2):
                for d in (1, 3, 2):
                    landed(hbuf.at[pl.ds(0, NXY), half], h2_recv.at[half, d])
        tot[...] = jnp.zeros_like(tot)

        def take(i, _):
            with scope("hdown"):
                landed(wd.at[0, pl.ds(i * NXY, NXY)], wd_sem.at[0, i])
                total = tot[...]
                for k in range(NXY):
                    units = hbuf[i * NXY + k].reshape(ROWS, UNITS)
                    block = jnp.dot(units, wd[0, i * NXY + k], preferred_element_type=jnp.float32)
                    total += block.astype(jnp.bfloat16).astype(jnp.float32)
                tot[...] = total
            return 0

        lax.fori_loop(0, NZ, take, 0)

    def gate_up(slot, l, n):
        pair = (NZ - 1 - n,)

        @pl.when(l > 0)
        def _():
            for i in pair:
                short = (i == 0) & (slot == 1) & runs_moved

                @pl.when(short)
                def _():
                    landed(xbuf.at[slot, pl.ds(0, NXY - 1)], ag_recv.at[slot, 0])

                @pl.when(jnp.logical_not(short))
                def _():
                    landed(xbuf.at[slot, pl.ds(i * NXY, NXY)], ag_recv.at[slot, i])

        def add(turned):
            squares = ssq[...]
            gate, up = accg[...], accu[...]
            which = lax.broadcasted_iota(jnp.int32, (4, 1), 0)
            for i in pair:
                cols = pl.ds(pl.multiple_of(shifted(table(i, TAKE_DZ)) * (NXY * BLK), NXY * BLK), NXY * BLK)
                gain = jnp.sum(jnp.where(which == l, gain_v[:, cols].astype(jnp.float32), 0.0), axis=0, keepdims=True)
                parts = []
                for k in range(NXY):
                    xf = xbuf[slot, i * NXY + k].astype(jnp.float32)
                    squares += xf * xf
                    parts.append((xf * gain[:, k * BLK:(k + 1) * BLK]).astype(jnp.bfloat16))
                lhs = jnp.concatenate(parts, axis=1)
                weights = wgt if turned else wg
                dims = (((1,), (0 if turned else 1,)), ((), ()))
                gate += lax.dot_general(lhs, weights[slot, i, 0], dims, preferred_element_type=jnp.float32)
                up += lax.dot_general(lhs, weights[slot, i, 1], dims, preferred_element_type=jnp.float32)
            ssq[...] = squares
            accg[...] = gate
            accu[...] = up

        pl.when(turns)(lambda: add(True))

        @pl.when(jnp.logical_not(turns))
        def _():
            for i in pair:
                landed(wg.at[slot, i], wg_sem.at[slot, i])
            add(False)

    def layer(slot, _):
        l = sec - 1 + slot
        to_group = table(l, next_group)
        to_slot = table(l, next_slot)
        stays = to_group == sec

        @pl.when(jnp.where(slot == 0, runs_moved, runs_own))
        def _():
            accg[...] = jnp.zeros_like(accg)
            accu[...] = jnp.zeros_like(accu)
            ssq[...] = jnp.zeros_like(ssq)
            def step(i, _):
                with scope("gu"):
                    gate_up(slot, l, i)
                return 0

            lax.fori_loop(0, NZ, step, 0)
            with scope("hid"):
                mean = jnp.sum(ssq[...], axis=1, keepdims=True) * (1.0 / (N * BLK))
                scale = lax.rsqrt(mean + NORM_EPS)
                gate = accg[...] * scale
                hidden = (gate / (1.0 + jnp.exp(-gate)) * (accu[...] * scale)).astype(jnp.bfloat16)
            pl.when(l == 0)(meet)
            def down(a, _):
                with scope("down"):
                    landed(wd.at[slot, pl.ds(a * NXY, NXY)], wd_sem.at[slot, a])
                    w = jnp.concatenate([wd[slot, a * NXY + k] for k in range(NXY)], axis=1)
                    part = jnp.dot(hidden, w, preferred_element_type=jnp.float32).astype(jnp.bfloat16)

                    @pl.when(l < 3)
                    def _():
                        for k in range(NXY):
                            ps[slot, a * NXY + k] = part[:, k * BLK:(k + 1) * BLK]
                        for k in range(NXY - 1):
                            rs_copy(slot, a, k).start()
                        pl.when(a < NZ - 1)(lambda: rs_copy(slot, a, NXY - 1).start())

                    @pl.when(l == 3)
                    def _():
                        zz = shifted(table(a, SEND_DZ))
                        for k, (dx, dy) in enumerate(XY):
                            cols = pl.ds(pl.multiple_of((zz * NXY + xs_of[dx] * NY + ys[dy]) * BLK, BLK), BLK)
                            prow[:, :, cols] = part[:, k * BLK:(k + 1) * BLK].reshape(ROWS // 2, 2, BLK)
                return 0

            def reduced_down():
                lax.fori_loop(0, NZ, down, 0)

                @pl.when(l < 3)
                def _():
                    rs[slot, NXY - 1] = ps[slot, N - 1]

                    def take(i, total):
                        pl.when(i == 0)(lambda: landed(rs.at[slot, pl.ds(0, NXY - 1)], rs_recv.at[slot, 0]))
                        pl.when(i > 0)(lambda: landed(rs.at[slot, pl.ds(i * NXY, NXY)], rs_recv.at[slot, i]))
                        for k in range(NXY):
                            total += rs[slot, i * NXY + k].astype(jnp.float32)
                        return total

                    with scope("sum"):
                        tot[...] = lax.fori_loop(0, NZ, take, jnp.zeros((ROWS, BLK), jnp.float32))

            if any_gather:
                by_units = gathers & (slot == 0)
                pl.when(by_units)(lambda: gathered_down(hidden))
                pl.when(jnp.logical_not(by_units))(reduced_down)
            else:
                reduced_down()

            @pl.when(l < 3)
            def _():
                new = (xbuf[slot, xy].astype(jnp.float32) + keep * tot[...]).astype(jnp.bfloat16)
                xs[slot] = new
                with scope("ag"):
                    def at_home(a, k):
                        @pl.when(stays)
                        def _():
                            xbuf[1, xy] = new

                        pl.when(jnp.logical_not(stays))(lambda: ag_copy(slot, to_group, to_slot, a, k).start())

                    peers(lambda a, k: ag_copy(slot, to_group, to_slot, a, k).start(), at_home)
                xpair[slot] = new.reshape(ROWS // 2, 2, BLK)
                with scope("pieces"):
                    pieces(slot, l)

            pl.when(l == 3)(finish_rows)
        return 0

    lax.fori_loop(0, 2, layer, 0)
    pl.when(sec == runs[0])(find_kept)

    comes = table(sec, source)
    with scope("rows"):
        for part in (0, 1):
            def wait_rows(count):
                landed(orow.at[part, :, pl.ds(0, count * BLK)], o_recv.at[part])

            here = (comes >= 0) & (sec < 3)
            if part:
                here = here & (z < NZ // 2)
            pl.when(here & (comes == sec))(lambda: wait_rows(N - 1))
            pl.when(here & (comes != sec))(lambda: wait_rows(N))

    @pl.when(comes < 0)
    def _():
        orow[0] = kept[0]

    @pl.when((comes < 0) | (z >= NZ // 2))
    def _():
        orow[1] = kept[1]

    with scope("assemble"):
        touched_full = comes >= 0
        touched_short = (comes >= 0) & (z < NZ // 2)
        for b in range(2):
            computed = jnp.where(full == b, orow[0].astype(jnp.float32), orow[1].astype(jnp.float32))
            use = jnp.where(full == b, jnp.where(touched_full, 1, 0), jnp.where(touched_short, 1, 0)) == 1
            out_ref[b] = jnp.where(use, computed, kept[b].astype(jnp.float32)).astype(jnp.bfloat16)

    def drain(slot, _):
        l = sec - 1 + slot
        to_group = table(l, next_group)
        to_slot = table(l, next_slot)
        stays = to_group == sec

        @pl.when(jnp.where(slot == 0, runs_moved, runs_own))
        def _():
            by_units = gathers & (slot == 0)
            pl.when(by_units)(lambda: landed(hbuf.at[pl.ds(0, N - 1)], h_send.at[0]))

            @pl.when(l < 3)
            def _():
                pl.when(jnp.logical_not(by_units))(lambda: landed(ps.at[slot, pl.ds(0, N - 1)], rs_send.at[slot]))
                pl.when(stays)(lambda: landed(ps.at[slot, pl.ds(0, N - 1)], ag_send.at[slot]))
                pl.when(jnp.logical_not(stays))(lambda: landed(ps.at[slot], ag_send.at[slot]))
                pieces_out(slot, l)

            @pl.when(l == 3)
            def _():
                landed(prow.at[pl.ds(0, N - 1)], p_send.at[0])
                pl.when(z < NZ // 2)(lambda: landed(prow.at[pl.ds(0, N // 2 - 1)], p_send.at[1]))
                pl.when(z >= NZ // 2)(lambda: landed(prow.at[pl.ds(0, N // 2)], p_send.at[1]))
        return 0

    with scope("drain"):
        lax.fori_loop(0, 2, drain, 0)
        pl.when(spreads)(lambda: landed(wd.at[0, pl.ds(0, N - 1)], rd_send.at[0]))


def relay(moved, counts, tokens, gains, w_in, w_out, b_in, b_out):
    bf, f32 = jnp.bfloat16, jnp.float32
    dma = pltpu.SemaphoreType.DMA
    anywhere = pl.BlockSpec(memory_space=pl.ANY)
    return pl.pallas_call(
        functools.partial(relay_kernel, moved),
        out_shape=jax.ShapeDtypeStruct((2, 2, N * BLK), bf),
        in_specs=[pl.BlockSpec(memory_space=pltpu.SMEM)] + [anywhere] * 6,
        out_specs=pl.BlockSpec(memory_space=pltpu.VMEM),
        scratch_shapes=[
            pltpu.VMEM((2, FULL, N * BLK), bf),
            pltpu.VMEM((4, N * BLK), bf),
            pltpu.VMEM((2, NZ, 2, UNITS, NXY * BLK), bf),
            pltpu.VMEM((2, NZ, 2, NXY * BLK, UNITS), bf),
            pltpu.VMEM((2, N, UNITS, BLK), bf),
            pltpu.VMEM((2, N, ROWS, BLK), bf),
            pltpu.VMEM((2, N, ROWS, BLK), bf),
            pltpu.VMEM((2, N, ROWS, BLK), bf),
            pltpu.VMEM((2, ROWS, BLK), bf),
            pltpu.VMEM((2, ROWS // 2, 2, BLK), bf),
            pltpu.VMEM((2, 2, N * BLK), bf),
            pltpu.VMEM((2, 2, N * BLK), bf),
            pltpu.VMEM((ROWS, UNITS), f32),
            pltpu.VMEM((ROWS, UNITS), f32),
            pltpu.VMEM((ROWS, BLK), f32),
            pltpu.VMEM((ROWS, BLK), f32),
            pltpu.VMEM((ROWS // 2, 2, N * BLK), bf),
            pltpu.VMEM((2, N, 2, N * BLK), bf),
            pltpu.VMEM((8, N * BLK), f32),
            pltpu.VMEM((N, 2, ROWS // 2, UNITS), bf),
            dma((2,)),
            dma((2, NZ)),
            dma((2, NZ)),
            dma((1,)),
            dma((2,)),
            dma((2, NZ)),
            dma((2,)),
            dma((2, NZ)),
            dma((2, 2, 2)),
            dma((2,)),
            dma((2,)),
            dma((2, NZ)),
            dma((1,)),
            dma((2, NXY)),
            dma((2, NZ)),
        ],
        compiler_params=pltpu.CompilerParams(
            collective_id=PLANS.index(moved), has_side_effects=True, vmem_limit_bytes=60 * 1024 * 1024
        ),
    )(counts, tokens, gains, w_in, w_out, b_in, b_out)


def shards(tokens, norm_gain, w_in, w_out, backup_in, backup_out, layer_group, token_counts):
    unmoved = sum(w * l for l, w in enumerate(PLAN_WEIGHTS))
    plan = jnp.sum(layer_group * jnp.array(PLAN_WEIGHTS, jnp.int32)) - (unmoved + 1)
    rows = lax.switch(
        plan,
        [functools.partial(relay, p) for p in PLANS],
        token_counts, tokens, norm_gain, w_in[0], w_out[0], backup_in[0], backup_out[0],
    )
    return rows[None]


def solution(mesh):
    finer = Mesh(mesh.devices.reshape(4, NZ, NX, NY), AXES)
    return jax.shard_map(
        shards,
        mesh=finer,
        in_specs=(
            P(),
            P(),
            P("section", None, TENSOR, None),
            P("section", TENSOR, None),
            P("section", None, TENSOR, None),
            P("section", None, TENSOR),
            P(),
            P(),
        ),
        out_specs=P("section", None, TENSOR, None),
        check_vma=False,
    )
```

```python
import functools

import jax
import jax.numpy as jnp
from jax import lax
from jax.experimental import pallas as pl
from jax.experimental.pallas import tpu as pltpu
from jax.sharding import Mesh
from jax.sharding import PartitionSpec as P

TENSOR = ("z", "xhi", "y")
AXES = ("section", "z", "xhi", "y")
MESH_ID = pl.DeviceIdType.MESH
NORM_EPS = 0.25
HOW = ("--R", "H--", "-H-", "-HH", "HR-", "HRH")
PLANS = ((0, 0, 1), (1, 0, 0), (0, 1, 0), (0, 1, 1), (1, 1, 0), (1, 1, 1))
PLAN_WEIGHTS = (2, 3, 1, 0)
NZ, NX, NY = 4, 2, 4
NXY = NX * NY
N = NZ * NXY
SEND_DZ = (2, 1, 3, 0)
TAKE_DZ = (0, 1, 3, 2)
XY = ((1, 2), (1, 1), (1, 3), (0, 2), (1, 0), (0, 1), (0, 3), (0, 0))
ZX = ((2, 1), (1, 1), (3, 1), (2, 0), (0, 1), (1, 0), (3, 0))
ZX_BACK = [ZX.index((-a % NZ, -b % NX)) for a, b in ZX]
XY_BACK = [XY.index((-b % NX, -c % NY)) for b, c in XY]
FULL, SHORT = 64, 32
ROWS = FULL + SHORT
HALF = ROWS // 2
BLK = 128
UNITS = 448


def table(index, values):
    out = jnp.int32(values[-1])
    for k in range(len(values) - 2, -1, -1):
        if values[k] != values[-1]:
            out = jnp.where(index == k, jnp.int32(values[k]), out)
    return out


def relay_kernel(
    moved,
    counts, tokens, gains, w_in, w_out, b_in, b_out,
    out_ref,
    tok_v, gain_v, wg, wgt, wd, xbuf, ps, rs, xs, xpair, orow, kept, accg, accu, ssq, tot, prow, rrow, xrow, hbuf,
    tok_sem, wg_sem, wd_sem, rd_send, rs_send, rs_recv, ag_send, ag_recv, o_send, o_recv, p_send, p_recv,
    h_send, h1_recv, h2_recv,
):
    m = tuple(moved) + (0,)
    runs = [l + m[l] for l in range(4)]
    reached = [sum(e <= g for e in runs) for g in range(4)]
    lost = moved.index(1)
    next_group = [runs[l + 1] if l < 3 else 0 for l in range(4)]
    next_slot = [1 - m[l + 1] if l < 3 else 0 for l in range(4)]
    own_out = [int(l < 3 and reached[runs[l]] == l + 1) for l in range(4)]
    lost_out = [int(lost > 0 and reached[lost] == l + 1) for l in range(4)]
    has_moved = [int(g > 0 and m[g - 1] == 1) for g in range(4)]
    has_own = [1 - m[g] for g in range(4)]
    source = [runs[r - 1] if r > 0 else -1 for r in reached]
    n_out = 2 if lost > 0 else 1
    how = HOW[PLANS.index(moved)]
    has_gather = [int(g > 0 and how[g - 1] == "H") for g in range(4)]
    has_spread = [int(g > 0 and how[g - 1] == "R") for g in range(4)]
    any_gather, any_spread = sum(has_gather) > 0, sum(has_spread) > 0

    sec = lax.axis_index("section")
    z, xh, y = (lax.axis_index(a) for a in TENSOR)
    xy = xh * NY + y
    me = z * NXY + xy
    zs = [lax.rem(z + d, NZ) for d in range(NZ)]
    xs_of = [lax.rem(xh + d, NX) for d in range(NX)]
    ys = [lax.rem(y + d, NY) for d in range(NY)]
    runs_moved = table(sec, has_moved) == 1
    runs_own = table(sec, has_own) == 1
    spreads = table(sec, has_spread) == 1
    gathers = table(sec, has_gather) == 1

    def shifted(dz):
        return lax.rem(z + dz, NZ)

    def scope(name):
        return jax.named_scope(name)

    tok_copy = pltpu.make_async_copy(tokens, tok_v, tok_sem.at[0])
    gain_copy = pltpu.make_async_copy(gains, gain_v, tok_sem.at[1])
    tok_copy.start()
    gain_copy.start()

    def load_in(slot, src):
        def go(n, _):
            i = NZ - 1 - n
            start = pl.multiple_of(shifted(table(i, TAKE_DZ)) * (NXY * BLK), NXY * BLK)
            for half in range(2):
                pltpu.make_async_copy(
                    src.at[half, :, pl.ds(start, NXY * BLK)], wg.at[slot, i, half], wg_sem.at[slot, i]
                ).start()
            return 0
        lax.fori_loop(0, NZ, go, 0)

    @pl.when(runs_moved)
    def _():
        load_in(0, b_in)

    @pl.when(runs_own)
    def _():
        load_in(1, w_in)

    barrier = pltpu.get_barrier_semaphore()

    def greet(n, _):
        g = table(n, [runs[0]] + [g for g in range(4) if g != runs[0]])
        for a in range(NZ):
            for k, (dx, dy) in enumerate(XY):
                def tell():
                    pl.semaphore_signal(
                        barrier, inc=1, device_id=(g, zs[SEND_DZ[a]], xs_of[dx], ys[dy]), device_id_type=MESH_ID
                    )

                if (a, k) == (NZ - 1, NXY - 1):
                    pl.when(g != sec)(tell)
                else:
                    tell()
        return 0

    with scope("greet"):
        lax.fori_loop(0, 4, greet, 0)

    if any_gather:
        @pl.when(gathers)
        def _():
            def go(i, _):
                for k in range(NXY):
                    block = i * NXY + k
                    start = pl.multiple_of(block * UNITS, UNITS)
                    pltpu.make_async_copy(b_out.at[pl.ds(start, UNITS), :], wd.at[0, block], wd_sem.at[0, i]).start()
                return 0
            lax.fori_loop(0, NZ, go, 0)

    @pl.when(runs_own)
    def _():
        def go(a, _):
            zz = shifted(table(a, SEND_DZ))
            for k, (dx, dy) in enumerate(XY):
                start = pl.multiple_of((zz * NXY + xs_of[dx] * NY + ys[dy]) * BLK, BLK)
                pltpu.make_async_copy(w_out.at[:, pl.ds(start, BLK)], wd.at[1, a * NXY + k], wd_sem.at[1, a]).start()
            return 0
        lax.fori_loop(0, NZ, go, 0)

    def spread(a, k):
        dx, dy = XY[k]
        zz = zs[SEND_DZ[a]]
        start = pl.multiple_of((zz * NXY + xs_of[dx] * NY + ys[dy]) * UNITS, UNITS)
        back = (0, 2, 1, 3)[a]
        return pltpu.make_async_remote_copy(
            src_ref=b_out.at[pl.ds(start, UNITS), :], dst_ref=wd.at[0, back * NXY + XY_BACK[k]],
            send_sem=rd_send.at[0], recv_sem=wd_sem.at[0, back],
            device_id=(sec, zz, xs_of[dx], ys[dy]), device_id_type=MESH_ID,
        )

    def landed(ref, sem):
        pltpu.make_async_copy(ref, ref, sem).wait()

    def peers(go, to_self=None):
        def step(a, _):
            for k in range(NXY):
                if k < NXY - 1:
                    go(a, k)
                else:
                    pl.when(a < NZ - 1)(lambda: go(a, k))
                    if to_self is not None:
                        pl.when(a == NZ - 1)(lambda: to_self(a, k))
            return 0
        lax.fori_loop(0, NZ, step, 0)

    def meet():
        with scope("barrier"):
            pl.semaphore_wait(barrier, 4 * N - 1)

        if any_spread:
            @pl.when(spreads)
            def _():
                with scope("redist"):
                    start = pl.multiple_of(me * UNITS, UNITS)
                    pltpu.make_async_copy(b_out.at[pl.ds(start, UNITS), :], wd.at[0, N - 1], wd_sem.at[0, NZ - 1]).start()
                    for n in range(NXY):
                        for a in range(NZ):
                            k = (n + 2 * a) % NXY
                            if (a, k) != (NZ - 1, NXY - 1):
                                spread(a, k).start()

    pl.when(sec != runs[0])(meet)

    full = jnp.where(counts[1] == FULL, 1, 0)
    short_count = jnp.where(full == 1, counts[0], counts[1])
    with scope("tokwait"):
        tok_copy.wait()
        gain_copy.wait()

    first_slot = 1 - m[0]

    @pl.when(sec == runs[0])
    def _():
        def go(i, _):
            zz = shifted(table(i, TAKE_DZ))
            for k in range(NXY):
                cols = pl.ds(pl.multiple_of((zz * NXY + k) * BLK, BLK), BLK)
                xbuf[first_slot, i * NXY + k, 0] = tok_v[full, 0:HALF, cols]
                xbuf[first_slot, i * NXY + k, 1, 0:FULL - HALF, :] = tok_v[full, HALF:FULL, cols]
                xbuf[first_slot, i * NXY + k, 1, FULL - HALF:HALF, :] = tok_v[1 - full, 0:SHORT, cols]
            return 0
        lax.fori_loop(0, NZ, go, 0)

    def find_kept():
        with scope("kept"):
            pick = lax.broadcasted_iota(jnp.int32, (8, FULL), 1) == me * 2 + lax.broadcasted_iota(jnp.int32, (8, FULL), 0)
            pick = jnp.where(pick, 1.0, 0.0).astype(jnp.bfloat16)
            for b in range(2):
                def go(c, _):
                    cols = pl.ds(pl.multiple_of(c * (NXY * BLK), NXY * BLK), NXY * BLK)
                    rows = jnp.dot(pick, tok_v[b, :, cols], preferred_element_type=jnp.float32)
                    kept[b, :, cols] = rows[0:2].astype(jnp.bfloat16)
                    return 0
                lax.fori_loop(0, NZ, go, 0)

    pl.when(sec != runs[0])(find_kept)

    turns = sec != runs[0]

    def turn(n, _):
        slot, half = n // (2 * NZ), lax.rem(n, 2)
        i = NZ - 1 - lax.rem(n, 2 * NZ) // 2

        @pl.when(jnp.where(slot == 0, runs_moved, runs_own))
        def _():
            pl.when(half == 0)(lambda: landed(wg.at[slot, i], wg_sem.at[slot, i]))
            with scope("turn"):
                wgt[slot, i, half] = wg[slot, i, half].T
        return 0

    @pl.when(turns)
    def _():
        lax.fori_loop(0, 4 * NZ, turn, 0)

    def rs_copy(slot, half, a, k):
        dx, dy = XY[k]
        return pltpu.make_async_remote_copy(
            src_ref=ps.at[slot, half, a * NXY + k], dst_ref=rs.at[slot, half, (NZ - 1 - a) * NXY + XY_BACK[k]],
            send_sem=rs_send.at[slot, half], recv_sem=rs_recv.at[slot, half, NZ - 1 - a],
            device_id=(sec, shifted(table(a, SEND_DZ)), xs_of[dx], ys[dy]), device_id_type=MESH_ID,
        )

    def ag_copy(slot, half, to_group, to_slot, a, k):
        dx, dy = XY[k]
        return pltpu.make_async_remote_copy(
            src_ref=xs.at[slot, half], dst_ref=xbuf.at[to_slot, (NZ - 1 - a) * NXY + xy, half],
            send_sem=ag_send.at[slot, half], recv_sem=ag_recv.at[to_slot, NZ - 1 - a],
            device_id=(to_group, shifted(table(a, SEND_DZ)), xs_of[dx], ys[dy]), device_id_type=MESH_ID,
        )

    def ag_whole(slot, to_group, to_slot, a, k):
        dx, dy = XY[k]
        return pltpu.make_async_remote_copy(
            src_ref=xs.at[slot], dst_ref=xbuf.at[to_slot, (NZ - 1 - a) * NXY + xy],
            send_sem=ag_send.at[slot, 1], recv_sem=ag_recv.at[to_slot, NZ - 1 - a],
            device_id=(to_group, shifted(table(a, SEND_DZ)), xs_of[dx], ys[dy]), device_id_type=MESH_ID,
        )

    def piece(slot, which, to_group, part, a, k):
        dx, dy = XY[k]
        zz = shifted(table(a, SEND_DZ))
        first = zz * NXY + xs_of[dx] * NY + ys[dy] + (FULL // 2 if part else 0)
        return pltpu.make_async_remote_copy(
            src_ref=xpair.at[slot, first], dst_ref=orow.at[part, :, pl.ds(pl.multiple_of(me * BLK, BLK), BLK)],
            send_sem=o_send.at[slot, which, part], recv_sem=o_recv.at[part],
            device_id=(to_group, zz, xs_of[dx], ys[dy]), device_id_type=MESH_ID,
        )

    def pieces(slot, l):
        def each(which, _):
            to_group = jnp.where(which == 0, sec, lost)
            wanted = jnp.where(which == 0, table(l, own_out), table(l, lost_out)) == 1

            def go(a, k):
                piece(slot, which, to_group, 0, a, k).start()
                pl.when(shifted(table(a, SEND_DZ)) < NZ // 2)(lambda: piece(slot, which, to_group, 1, a, k).start())

            def to_self(a, k):
                pl.when(which == 1)(lambda: go(a, k))

                @pl.when(which == 0)
                def _():
                    cols = pl.ds(pl.multiple_of(me * BLK, BLK), BLK)
                    orow[0, :, cols] = xpair[slot, me]

                    @pl.when(z < NZ // 2)
                    def _():
                        orow[1, :, cols] = xpair[slot, FULL // 2 + me]

            pl.when(wanted)(lambda: peers(go, to_self))
            return 0

        lax.fori_loop(0, n_out, each, 0)

    def pieces_out(slot, l):
        half = N // 2
        for which in range(n_out):
            @pl.when(table(l, lost_out if which else own_out) == 1)
            def _():
                if which:
                    landed(xpair.at[slot, pl.ds(0, N)], o_send.at[slot, which, 0])
                    landed(xpair.at[slot, pl.ds(0, half)], o_send.at[slot, which, 1])
                else:
                    landed(xpair.at[slot, pl.ds(0, N - 1)], o_send.at[slot, which, 0])
                    pl.when(z < NZ // 2)(lambda: landed(xpair.at[slot, pl.ds(0, half - 1)], o_send.at[slot, which, 1]))
                    pl.when(z >= NZ // 2)(lambda: landed(xpair.at[slot, pl.ds(0, half)], o_send.at[slot, which, 1]))

    def row_copy(part, a, k):
        dx, dy = XY[k]
        zz = shifted(table(a, SEND_DZ))
        first = zz * NXY + xs_of[dx] * NY + ys[dy] + (FULL // 2 if part else 0)
        return pltpu.make_async_remote_copy(
            src_ref=prow.at[first], dst_ref=rrow.at[part, (NZ - 1 - a) * NXY + XY_BACK[k]],
            send_sem=p_send.at[part], recv_sem=p_recv.at[part, NZ - 1 - a],
            device_id=(sec, zz, xs_of[dx], ys[dy]), device_id_type=MESH_ID,
        )

    def finish_rows():
        with scope("rowsend"):
            def go(a, k):
                row_copy(0, a, k).start()
                pl.when(shifted(table(a, SEND_DZ)) < NZ // 2)(lambda: row_copy(1, a, k).start())

            peers(go)
        with scope("rowpick"):
            r = lax.broadcasted_iota(jnp.int32, (8, ROWS), 0)
            c = lax.broadcasted_iota(jnp.int32, (8, ROWS), 1)
            pick = jnp.where(c == me * 2 + jnp.where(r < 2, r, r - 2 + FULL), 1.0, 0.0)
            pick = jnp.where((r < 2) | (z < NZ // 2), pick, 0.0).astype(jnp.bfloat16)

            def fetch(i, _):
                cols = pl.ds(pl.multiple_of(shifted(table(i, TAKE_DZ)) * (NXY * BLK), NXY * BLK), NXY * BLK)
                x = jnp.concatenate([xbuf[1, i * NXY + k].reshape(ROWS, BLK) for k in range(NXY)], axis=1)
                xrow[:, cols] = jnp.dot(pick, x, preferred_element_type=jnp.float32)
                return 0

            lax.fori_loop(0, NZ, fetch, 0)
            rrow[0, N // NZ - 1] = prow[me]

            @pl.when(z < NZ // 2)
            def _():
                rrow[1, N // NZ - 1] = prow[FULL // 2 + me]

        def total_of(part):
            def take(i, total):
                pl.when(i == 0)(lambda: landed(rrow.at[part, pl.ds(0, NXY - 1)], p_recv.at[part, 0]))
                pl.when(i > 0)(lambda: landed(rrow.at[part, pl.ds(i * NXY, NXY)], p_recv.at[part, i]))
                for k in range(NXY):
                    total += rrow[part, i * NXY + k].astype(jnp.float32)
                return total
            return lax.fori_loop(0, NZ, take, jnp.zeros((2, N * BLK), jnp.float32))

        with scope("rowsum"):
            orow[0] = (xrow[0:2, :] + total_of(0)).astype(jnp.bfloat16)

            @pl.when(z < NZ // 2)
            def _():
                r = lax.broadcasted_iota(jnp.int32, (2, 1), 0) + me * 2
                orow[1] = (xrow[2:4, :] + jnp.where(r < short_count, 1.0, 0.0) * total_of(1)).astype(jnp.bfloat16)

    def half_block(half, src, to, recv):
        return pltpu.make_async_remote_copy(
            src_ref=hbuf.at[src, half], dst_ref=hbuf.at[src, half], send_sem=h_send.at[0], recv_sem=recv,
            device_id=(sec, *to), device_id_type=MESH_ID,
        )

    def along_z(src):
        for d in (2, 1, 3):
            half_block(0, src, (zs[d], xh, y), h2_recv.at[0, (-d) % NZ]).start()

    def along_y(src):
        for d in (2, 1, 3):
            half_block(1, src, (z, xh, ys[d]), h2_recv.at[1, (-d) % NY]).start()

    def gathered_down(hidden):
        hbuf[me] = hidden.reshape(2, ROWS // 2, UNITS)
        with scope("hsend"):
            for k in range(NXY - 1):
                dx, dy = XY[k]
                half_block(0, me, (z, xs_of[dx], ys[dy]), h1_recv.at[0, XY_BACK[k]]).start()
                dz, dx = ZX[k]
                half_block(1, me, (zs[dz], xs_of[dx], y), h1_recv.at[1, ZX_BACK[k]]).start()
            along_z(me)
            along_y(me)
        with scope("hforward"):
            for k in range(NXY - 2, -1, -1):
                dx, dy = XY[k]
                src = z * NXY + xs_of[dx] * NY + ys[dy]
                landed(hbuf.at[src, 0], h1_recv.at[0, k])
                along_z(src)
                dz, dx = ZX[k]
                src = zs[dz] * NXY + xs_of[dx] * NY + y
                landed(hbuf.at[src, 1], h1_recv.at[1, k])
                along_y(src)
        with scope("hwait"):
            for half in range(2):
                for d in (1, 3, 2):
                    landed(hbuf.at[pl.ds(0, NXY), half], h2_recv.at[half, d])
        tot[...] = jnp.zeros_like(tot)

        def take(i, _):
            with scope("hdown"):
                landed(wd.at[0, pl.ds(i * NXY, NXY)], wd_sem.at[0, i])
                total = tot[...].reshape(ROWS, BLK)
                for k in range(NXY):
                    units = hbuf[i * NXY + k].reshape(ROWS, UNITS)
                    block = jnp.dot(units, wd[0, i * NXY + k], preferred_element_type=jnp.float32)
                    total += block.astype(jnp.bfloat16).astype(jnp.float32)
                tot[...] = total.reshape(2, HALF, BLK)
            return 0

        lax.fori_loop(0, NZ, take, 0)

    def gate_up(slot, l, n):
        pair = (NZ - 1 - n,)

        @pl.when(l > 0)
        def _():
            for i in pair:
                short = (i == 0) & (slot == 1) & runs_moved

                @pl.when(short)
                def _():
                    landed(xbuf.at[slot, pl.ds(0, NXY - 1)], ag_recv.at[slot, 0])

                @pl.when(jnp.logical_not(short))
                def _():
                    landed(xbuf.at[slot, pl.ds(i * NXY, NXY)], ag_recv.at[slot, i])

        def add(turned):
            squares = ssq[...]
            gate, up = accg[...], accu[...]
            which = lax.broadcasted_iota(jnp.int32, (4, 1), 0)
            for i in pair:
                cols = pl.ds(pl.multiple_of(shifted(table(i, TAKE_DZ)) * (NXY * BLK), NXY * BLK), NXY * BLK)
                gain = jnp.sum(jnp.where(which == l, gain_v[:, cols].astype(jnp.float32), 0.0), axis=0, keepdims=True)
                parts = []
                for k in range(NXY):
                    xf = xbuf[slot, i * NXY + k].reshape(ROWS, BLK).astype(jnp.float32)
                    squares += xf * xf
                    parts.append((xf * gain[:, k * BLK:(k + 1) * BLK]).astype(jnp.bfloat16))
                lhs = jnp.concatenate(parts, axis=1)
                weights = wgt if turned else wg
                dims = (((1,), (0 if turned else 1,)), ((), ()))
                gate += lax.dot_general(lhs, weights[slot, i, 0], dims, preferred_element_type=jnp.float32)
                up += lax.dot_general(lhs, weights[slot, i, 1], dims, preferred_element_type=jnp.float32)
            ssq[...] = squares
            accg[...] = gate
            accu[...] = up

        pl.when(turns)(lambda: add(True))

        @pl.when(jnp.logical_not(turns))
        def _():
            for i in pair:
                landed(wg.at[slot, i], wg_sem.at[slot, i])
            add(False)

    def layer(slot, _):
        l = sec - 1 + slot
        to_group = table(l, next_group)
        to_slot = table(l, next_slot)
        stays = to_group == sec

        @pl.when(jnp.where(slot == 0, runs_moved, runs_own))
        def _():
            accg[...] = jnp.zeros_like(accg)
            accu[...] = jnp.zeros_like(accu)
            ssq[...] = jnp.zeros_like(ssq)
            def step(i, _):
                with scope("gu"):
                    gate_up(slot, l, i)
                return 0

            lax.fori_loop(0, NZ, step, 0)
            with scope("hid"):
                mean = jnp.sum(ssq[...], axis=1, keepdims=True) * (1.0 / (N * BLK))
                scale = lax.rsqrt(mean + NORM_EPS)
                gate = accg[...] * scale
                hidden = (gate / (1.0 + jnp.exp(-gate)) * (accu[...] * scale)).astype(jnp.bfloat16)
            pl.when(l == 0)(meet)
            def down(a, _):
                with scope("down"):
                    landed(wd.at[slot, pl.ds(a * NXY, NXY)], wd_sem.at[slot, a])
                    w = jnp.concatenate([wd[slot, a * NXY + k] for k in range(NXY)], axis=1)
                    part = jnp.dot(hidden, w, preferred_element_type=jnp.float32).astype(jnp.bfloat16)

                    @pl.when(l < 3)
                    def _():
                        for k in range(NXY):
                            for half in range(2):
                                ps[slot, half, a * NXY + k] = part[half * HALF:(half + 1) * HALF, k * BLK:(k + 1) * BLK]
                        for k in range(NXY - 1):
                            rs_copy(slot, 0, a, k).start()
                        pl.when(a < NZ - 1)(lambda: rs_copy(slot, 0, a, NXY - 1).start())

                    @pl.when(l == 3)
                    def _():
                        zz = shifted(table(a, SEND_DZ))
                        for k, (dx, dy) in enumerate(XY):
                            cols = pl.ds(pl.multiple_of((zz * NXY + xs_of[dx] * NY + ys[dy]) * BLK, BLK), BLK)
                            prow[:, :, cols] = part[:, k * BLK:(k + 1) * BLK].reshape(ROWS // 2, 2, BLK)
                return 0

            def reduced_down():
                lax.fori_loop(0, NZ, down, 0)

                @pl.when(l < 3)
                def _():
                    peers(lambda a, k: rs_copy(slot, 1, a, k).start())
                    for half in range(2):
                        rs[slot, half, NXY - 1] = ps[slot, half, N - 1]

            by_units = gathers & (slot == 0)
            if any_gather:
                pl.when(by_units)(lambda: gathered_down(hidden))
                pl.when(jnp.logical_not(by_units))(reduced_down)
            else:
                reduced_down()

            def pass_on(half, _):
                @pl.when(jnp.logical_not(by_units))
                def _():
                    def take(i, total):
                        pl.when(i == 0)(lambda: landed(rs.at[slot, half, pl.ds(0, NXY - 1)], rs_recv.at[slot, half, 0]))
                        pl.when(i > 0)(lambda: landed(rs.at[slot, half, pl.ds(i * NXY, NXY)], rs_recv.at[slot, half, i]))
                        for k in range(NXY):
                            total += rs[slot, half, i * NXY + k].astype(jnp.float32)
                        return total

                    with scope("sum"):
                        tot[half] = lax.fori_loop(0, NZ, take, jnp.zeros((HALF, BLK), jnp.float32))

                row = lax.broadcasted_iota(jnp.int32, (HALF, 1), 0) + half * HALF
                keep = jnp.where(row < FULL + short_count, 1.0, 0.0)
                new = (xbuf[slot, xy, half].astype(jnp.float32) + keep * tot[half]).astype(jnp.bfloat16)
                xs[slot, half] = new

                @pl.when(stays)
                def _():
                    xbuf[1, xy, half] = new

                def send(copy):
                    def at_home(a, k):
                        pl.when(jnp.logical_not(stays))(lambda: copy(a, k).start())

                    peers(lambda a, k: copy(a, k).start(), at_home)

                with scope("ag"):
                    if any_gather:
                        pl.when(jnp.logical_not(by_units))(
                            lambda: send(lambda a, k: ag_copy(slot, half, to_group, to_slot, a, k))
                        )
                        pl.when(by_units & (half == 1))(
                            lambda: send(lambda a, k: ag_whole(slot, to_group, to_slot, a, k))
                        )
                    else:
                        send(lambda a, k: ag_copy(slot, half, to_group, to_slot, a, k))
                xpair[slot, pl.ds(half * (HALF // 2), HALF // 2)] = new.reshape(HALF // 2, 2, BLK)
                return 0

            @pl.when(l < 3)
            def _():
                lax.fori_loop(0, 2, pass_on, 0)
                with scope("pieces"):
                    pieces(slot, l)

            pl.when(l == 3)(finish_rows)
        return 0

    lax.fori_loop(0, 2, layer, 0)
    pl.when(sec == runs[0])(find_kept)

    comes = table(sec, source)
    with scope("rows"):
        for part in (0, 1):
            def wait_rows(count):
                landed(orow.at[part, :, pl.ds(0, count * BLK)], o_recv.at[part])

            here = (comes >= 0) & (sec < 3)
            if part:
                here = here & (z < NZ // 2)
            pl.when(here & (comes == sec))(lambda: wait_rows(N - 1))
            pl.when(here & (comes != sec))(lambda: wait_rows(N))

    @pl.when(comes < 0)
    def _():
        orow[0] = kept[0]

    @pl.when((comes < 0) | (z >= NZ // 2))
    def _():
        orow[1] = kept[1]

    with scope("assemble"):
        touched_full = comes >= 0
        touched_short = (comes >= 0) & (z < NZ // 2)
        for b in range(2):
            computed = jnp.where(full == b, orow[0].astype(jnp.float32), orow[1].astype(jnp.float32))
            use = jnp.where(full == b, jnp.where(touched_full, 1, 0), jnp.where(touched_short, 1, 0)) == 1
            out_ref[b] = jnp.where(use, computed, kept[b].astype(jnp.float32)).astype(jnp.bfloat16)

    def drain(slot, _):
        l = sec - 1 + slot
        to_group = table(l, next_group)
        to_slot = table(l, next_slot)
        stays = to_group == sec

        @pl.when(jnp.where(slot == 0, runs_moved, runs_own))
        def _():
            by_units = gathers & (slot == 0)
            pl.when(by_units)(lambda: landed(hbuf.at[pl.ds(0, N - 1)], h_send.at[0]))

            @pl.when(l < 3)
            def _():
                @pl.when(jnp.logical_not(by_units))
                def _():
                    for half in range(2):
                        sent = ps.at[slot, half, pl.ds(0, N - 1)]
                        landed(sent, rs_send.at[slot, half])
                        pl.when(stays)(lambda: landed(sent, ag_send.at[slot, half]))
                        pl.when(jnp.logical_not(stays))(lambda: landed(ps.at[slot, half], ag_send.at[slot, half]))

                @pl.when(by_units)
                def _():
                    pl.when(stays)(lambda: landed(xbuf.at[slot, pl.ds(0, N - 1)], ag_send.at[slot, 1]))
                    pl.when(jnp.logical_not(stays))(lambda: landed(xbuf.at[slot], ag_send.at[slot, 1]))

                pieces_out(slot, l)

            @pl.when(l == 3)
            def _():
                landed(prow.at[pl.ds(0, N - 1)], p_send.at[0])
                pl.when(z < NZ // 2)(lambda: landed(prow.at[pl.ds(0, N // 2 - 1)], p_send.at[1]))
                pl.when(z >= NZ // 2)(lambda: landed(prow.at[pl.ds(0, N // 2)], p_send.at[1]))
        return 0

    with scope("drain"):
        lax.fori_loop(0, 2, drain, 0)
        pl.when(spreads)(lambda: landed(wd.at[0, pl.ds(0, N - 1)], rd_send.at[0]))


def relay(moved, counts, tokens, gains, w_in, w_out, b_in, b_out):
    bf, f32 = jnp.bfloat16, jnp.float32
    dma = pltpu.SemaphoreType.DMA
    anywhere = pl.BlockSpec(memory_space=pl.ANY)
    return pl.pallas_call(
        functools.partial(relay_kernel, moved),
        out_shape=jax.ShapeDtypeStruct((2, 2, N * BLK), bf),
        in_specs=[pl.BlockSpec(memory_space=pltpu.SMEM)] + [anywhere] * 6,
        out_specs=pl.BlockSpec(memory_space=pltpu.VMEM),
        scratch_shapes=[
            pltpu.VMEM((2, FULL, N * BLK), bf),
            pltpu.VMEM((4, N * BLK), bf),
            pltpu.VMEM((2, NZ, 2, UNITS, NXY * BLK), bf),
            pltpu.VMEM((2, NZ, 2, NXY * BLK, UNITS), bf),
            pltpu.VMEM((2, N, UNITS, BLK), bf),
            pltpu.VMEM((2, N, 2, HALF, BLK), bf),
            pltpu.VMEM((2, 2, N, HALF, BLK), bf),
            pltpu.VMEM((2, 2, N, HALF, BLK), bf),
            pltpu.VMEM((2, 2, HALF, BLK), bf),
            pltpu.VMEM((2, ROWS // 2, 2, BLK), bf),
            pltpu.VMEM((2, 2, N * BLK), bf),
            pltpu.VMEM((2, 2, N * BLK), bf),
            pltpu.VMEM((ROWS, UNITS), f32),
            pltpu.VMEM((ROWS, UNITS), f32),
            pltpu.VMEM((ROWS, BLK), f32),
            pltpu.VMEM((2, HALF, BLK), f32),
            pltpu.VMEM((ROWS // 2, 2, N * BLK), bf),
            pltpu.VMEM((2, N, 2, N * BLK), bf),
            pltpu.VMEM((8, N * BLK), f32),
            pltpu.VMEM((N, 2, ROWS // 2, UNITS), bf),
            dma((2,)),
            dma((2, NZ)),
            dma((2, NZ)),
            dma((1,)),
            dma((2, 2)),
            dma((2, 2, NZ)),
            dma((2, 2)),
            dma((2, NZ)),
            dma((2, 2, 2)),
            dma((2,)),
            dma((2,)),
            dma((2, NZ)),
            dma((1,)),
            dma((2, NXY)),
            dma((2, NZ)),
        ],
        compiler_params=pltpu.CompilerParams(
            collective_id=PLANS.index(moved), has_side_effects=True, vmem_limit_bytes=60 * 1024 * 1024
        ),
    )(counts, tokens, gains, w_in, w_out, b_in, b_out)


def shards(tokens, norm_gain, w_in, w_out, backup_in, backup_out, layer_group, token_counts):
    unmoved = sum(w * l for l, w in enumerate(PLAN_WEIGHTS))
    plan = jnp.sum(layer_group * jnp.array(PLAN_WEIGHTS, jnp.int32)) - (unmoved + 1)
    rows = lax.switch(
        plan,
        [functools.partial(relay, p) for p in PLANS],
        token_counts, tokens, norm_gain, w_in[0], w_out[0], backup_in[0], backup_out[0],
    )
    return rows[None]


def solution(mesh):
    finer = Mesh(mesh.devices.reshape(4, NZ, NX, NY), AXES)
    return jax.shard_map(
        shards,
        mesh=finer,
        in_specs=(
            P(),
            P(),
            P("section", None, TENSOR, None),
            P("section", TENSOR, None),
            P("section", None, TENSOR, None),
            P("section", None, TENSOR),
            P(),
            P(),
        ),
        out_specs=P("section", None, TENSOR, None),
        check_vma=False,
    )
```

```python
import functools

import jax
import jax.numpy as jnp
from jax import lax
from jax.experimental import pallas as pl
from jax.experimental.pallas import tpu as pltpu
from jax.sharding import Mesh
from jax.sharding import PartitionSpec as P

TENSOR = ("z", "xhi", "y")
AXES = ("section", "z", "xhi", "y")
MESH_ID = pl.DeviceIdType.MESH
NORM_EPS = 0.25
HOW = ("--R", "H--", "-H-", "-HH", "HR-", "HRH")
PLANS = ((0, 0, 1), (1, 0, 0), (0, 1, 0), (0, 1, 1), (1, 1, 0), (1, 1, 1))
PLAN_WEIGHTS = (2, 3, 1, 0)
NZ, NX, NY = 4, 2, 4
NXY = NX * NY
N = NZ * NXY
SEND_DZ = (2, 1, 3, 0)
TAKE_DZ = (0, 1, 3, 2)
XY = ((1, 2), (1, 1), (1, 3), (0, 2), (1, 0), (0, 1), (0, 3), (0, 0))
ZX = ((2, 1), (1, 1), (3, 1), (2, 0), (0, 1), (1, 0), (3, 0))
ZX_BACK = [ZX.index((-a % NZ, -b % NX)) for a, b in ZX]
XY_BACK = [XY.index((-b % NX, -c % NY)) for b, c in XY]
FULL, SHORT = 64, 32
ROWS = FULL + SHORT
HALF = ROWS // 2
BLK = 128
UNITS = 448


def table(index, values):
    out = jnp.int32(values[-1])
    for k in range(len(values) - 2, -1, -1):
        if values[k] != values[-1]:
            out = jnp.where(index == k, jnp.int32(values[k]), out)
    return out


def relay_kernel(
    moved,
    counts, tokens, gains, w_in, w_out, b_in, b_out,
    out_ref,
    tok_v, gain_v, wg, wgt, wd, xbuf, ps, rs, xs, xpair, orow, kept, accg, accu, ssq, tot, prow, rrow, xrow, hbuf,
    tok_sem, wg_sem, wd_sem, rd_send, rs_send, rs_recv, ag_send, ag_recv, o_send, o_recv, p_send, p_recv,
    h_send, h1_recv, h2_recv,
):
    m = tuple(moved) + (0,)
    runs = [l + m[l] for l in range(4)]
    reached = [sum(e <= g for e in runs) for g in range(4)]
    lost = moved.index(1)
    next_group = [runs[l + 1] if l < 3 else 0 for l in range(4)]
    next_slot = [1 - m[l + 1] if l < 3 else 0 for l in range(4)]
    own_out = [int(l < 3 and reached[runs[l]] == l + 1) for l in range(4)]
    lost_out = [int(lost > 0 and reached[lost] == l + 1) for l in range(4)]
    has_moved = [int(g > 0 and m[g - 1] == 1) for g in range(4)]
    has_own = [1 - m[g] for g in range(4)]
    source = [runs[r - 1] if r > 0 else -1 for r in reached]
    n_out = 2 if lost > 0 else 1
    how = HOW[PLANS.index(moved)]
    has_gather = [int(g > 0 and how[g - 1] == "H") for g in range(4)]
    has_spread = [int(g > 0 and how[g - 1] == "R") for g in range(4)]
    any_gather, any_spread = sum(has_gather) > 0, sum(has_spread) > 0

    sec = lax.axis_index("section")
    z, xh, y = (lax.axis_index(a) for a in TENSOR)
    xy = xh * NY + y
    me = z * NXY + xy
    zs = [lax.rem(z + d, NZ) for d in range(NZ)]
    xs_of = [lax.rem(xh + d, NX) for d in range(NX)]
    ys = [lax.rem(y + d, NY) for d in range(NY)]
    runs_moved = table(sec, has_moved) == 1
    runs_own = table(sec, has_own) == 1
    spreads = table(sec, has_spread) == 1
    gathers = table(sec, has_gather) == 1

    def shifted(dz):
        return lax.rem(z + dz, NZ)

    def scope(name):
        return jax.named_scope(name)

    tok_copy = pltpu.make_async_copy(tokens, tok_v, tok_sem.at[0])
    gain_copy = pltpu.make_async_copy(gains, gain_v, tok_sem.at[1])
    tok_copy.start()
    gain_copy.start()

    def load_in(slot, src):
        def go(n, _):
            i = NZ - 1 - n
            start = pl.multiple_of(shifted(table(i, TAKE_DZ)) * (NXY * BLK), NXY * BLK)
            for half in range(2):
                pltpu.make_async_copy(
                    src.at[half, :, pl.ds(start, NXY * BLK)], wg.at[slot, i, half], wg_sem.at[slot, i]
                ).start()
            return 0
        lax.fori_loop(0, NZ, go, 0)

    @pl.when(runs_moved)
    def _():
        load_in(0, b_in)

    @pl.when(runs_own)
    def _():
        load_in(1, w_in)

    barrier = pltpu.get_barrier_semaphore()

    def greet(n, _):
        g = table(n, [runs[0]] + [g for g in range(4) if g != runs[0]])
        for a in range(NZ):
            for k, (dx, dy) in enumerate(XY):
                def tell():
                    pl.semaphore_signal(
                        barrier, inc=1, device_id=(g, zs[SEND_DZ[a]], xs_of[dx], ys[dy]), device_id_type=MESH_ID
                    )

                if (a, k) == (NZ - 1, NXY - 1):
                    pl.when(g != sec)(tell)
                else:
                    tell()
        return 0

    with scope("greet"):
        lax.fori_loop(0, 4, greet, 0)

    if any_gather:
        @pl.when(gathers)
        def _():
            def go(i, _):
                for k in range(NXY):
                    block = i * NXY + k
                    start = pl.multiple_of(block * UNITS, UNITS)
                    pltpu.make_async_copy(b_out.at[pl.ds(start, UNITS), :], wd.at[0, block], wd_sem.at[0, i]).start()
                return 0
            lax.fori_loop(0, NZ, go, 0)

    @pl.when(runs_own)
    def _():
        def go(a, _):
            zz = shifted(table(a, SEND_DZ))
            for k, (dx, dy) in enumerate(XY):
                start = pl.multiple_of((zz * NXY + xs_of[dx] * NY + ys[dy]) * BLK, BLK)
                pltpu.make_async_copy(w_out.at[:, pl.ds(start, BLK)], wd.at[1, a * NXY + k], wd_sem.at[1, a]).start()
            return 0
        lax.fori_loop(0, NZ, go, 0)

    def spread(a, k):
        dx, dy = XY[k]
        zz = zs[SEND_DZ[a]]
        start = pl.multiple_of((zz * NXY + xs_of[dx] * NY + ys[dy]) * UNITS, UNITS)
        back = (0, 2, 1, 3)[a]
        return pltpu.make_async_remote_copy(
            src_ref=b_out.at[pl.ds(start, UNITS), :], dst_ref=wd.at[0, back * NXY + XY_BACK[k]],
            send_sem=rd_send.at[0], recv_sem=wd_sem.at[0, back],
            device_id=(sec, zz, xs_of[dx], ys[dy]), device_id_type=MESH_ID,
        )

    def landed(ref, sem):
        pltpu.make_async_copy(ref, ref, sem).wait()

    def peers(go, to_self=None):
        def step(a, _):
            for k in range(NXY):
                if k < NXY - 1:
                    go(a, k)
                else:
                    pl.when(a < NZ - 1)(lambda: go(a, k))
                    if to_self is not None:
                        pl.when(a == NZ - 1)(lambda: to_self(a, k))
            return 0
        lax.fori_loop(0, NZ, step, 0)

    def meet():
        with scope("barrier"):
            pl.semaphore_wait(barrier, 4 * N - 1)

        if any_spread:
            @pl.when(spreads)
            def _():
                with scope("redist"):
                    start = pl.multiple_of(me * UNITS, UNITS)
                    pltpu.make_async_copy(b_out.at[pl.ds(start, UNITS), :], wd.at[0, N - 1], wd_sem.at[0, NZ - 1]).start()
                    for n in range(NXY):
                        for a in range(NZ):
                            k = (n + 2 * a) % NXY
                            if (a, k) != (NZ - 1, NXY - 1):
                                spread(a, k).start()

    pl.when(sec != runs[0])(meet)

    full = jnp.where(counts[1] == FULL, 1, 0)
    short_count = jnp.where(full == 1, counts[0], counts[1])
    with scope("tokwait"):
        tok_copy.wait()
        gain_copy.wait()

    first_slot = 1 - m[0]

    @pl.when(sec == runs[0])
    def _():
        def go(i, _):
            zz = shifted(table(i, TAKE_DZ))
            for k in range(NXY):
                cols = pl.ds(pl.multiple_of((zz * NXY + k) * BLK, BLK), BLK)
                xbuf[first_slot, i * NXY + k, 0] = tok_v[full, 0:HALF, cols]
                xbuf[first_slot, i * NXY + k, 1, 0:FULL - HALF, :] = tok_v[full, HALF:FULL, cols]
                xbuf[first_slot, i * NXY + k, 1, FULL - HALF:HALF, :] = tok_v[1 - full, 0:SHORT, cols]
            return 0
        lax.fori_loop(0, NZ, go, 0)

    def find_kept():
        with scope("kept"):
            pick = lax.broadcasted_iota(jnp.int32, (8, FULL), 1) == me * 2 + lax.broadcasted_iota(jnp.int32, (8, FULL), 0)
            pick = jnp.where(pick, 1.0, 0.0).astype(jnp.bfloat16)
            for b in range(2):
                def go(c, _):
                    cols = pl.ds(pl.multiple_of(c * (NXY * BLK), NXY * BLK), NXY * BLK)
                    rows = jnp.dot(pick, tok_v[b, :, cols], preferred_element_type=jnp.float32)
                    kept[b, :, cols] = rows[0:2].astype(jnp.bfloat16)
                    return 0
                lax.fori_loop(0, NZ, go, 0)

    pl.when(sec != runs[0])(find_kept)

    turns = sec != runs[0]

    def turn(n, _):
        slot, half = n // (2 * NZ), lax.rem(n, 2)
        i = NZ - 1 - lax.rem(n, 2 * NZ) // 2

        @pl.when(jnp.where(slot == 0, runs_moved, runs_own))
        def _():
            pl.when(half == 0)(lambda: landed(wg.at[slot, i], wg_sem.at[slot, i]))
            with scope("turn"):
                wgt[slot, i, half] = wg[slot, i, half].T
        return 0

    @pl.when(turns)
    def _():
        lax.fori_loop(0, 4 * NZ, turn, 0)

    def rs_copy(slot, half, a, k):
        dx, dy = XY[k]
        return pltpu.make_async_remote_copy(
            src_ref=ps.at[slot, half, a * NXY + k], dst_ref=rs.at[slot, half, (NZ - 1 - a) * NXY + XY_BACK[k]],
            send_sem=rs_send.at[slot, half], recv_sem=rs_recv.at[slot, half, NZ - 1 - a],
            device_id=(sec, shifted(table(a, SEND_DZ)), xs_of[dx], ys[dy]), device_id_type=MESH_ID,
        )

    def ag_copy(slot, half, to_group, to_slot, a, k):
        dx, dy = XY[k]
        return pltpu.make_async_remote_copy(
            src_ref=xs.at[slot, half], dst_ref=xbuf.at[to_slot, (NZ - 1 - a) * NXY + xy, half],
            send_sem=ag_send.at[slot, half], recv_sem=ag_recv.at[to_slot, NZ - 1 - a],
            device_id=(to_group, shifted(table(a, SEND_DZ)), xs_of[dx], ys[dy]), device_id_type=MESH_ID,
        )

    def ag_whole(slot, to_group, to_slot, a, k):
        dx, dy = XY[k]
        return pltpu.make_async_remote_copy(
            src_ref=xs.at[slot], dst_ref=xbuf.at[to_slot, (NZ - 1 - a) * NXY + xy],
            send_sem=ag_send.at[slot, 1], recv_sem=ag_recv.at[to_slot, NZ - 1 - a],
            device_id=(to_group, shifted(table(a, SEND_DZ)), xs_of[dx], ys[dy]), device_id_type=MESH_ID,
        )

    def piece(slot, which, to_group, part, a, k):
        dx, dy = XY[k]
        zz = shifted(table(a, SEND_DZ))
        first = zz * NXY + xs_of[dx] * NY + ys[dy] + (FULL // 2 if part else 0)
        return pltpu.make_async_remote_copy(
            src_ref=xpair.at[slot, first], dst_ref=orow.at[part, :, pl.ds(pl.multiple_of(me * BLK, BLK), BLK)],
            send_sem=o_send.at[slot, which, part], recv_sem=o_recv.at[part],
            device_id=(to_group, zz, xs_of[dx], ys[dy]), device_id_type=MESH_ID,
        )

    def pieces(slot, l):
        def each(which, _):
            to_group = jnp.where(which == 0, sec, lost)
            wanted = jnp.where(which == 0, table(l, own_out), table(l, lost_out)) == 1

            def go(a, k):
                piece(slot, which, to_group, 0, a, k).start()
                pl.when(shifted(table(a, SEND_DZ)) < NZ // 2)(lambda: piece(slot, which, to_group, 1, a, k).start())

            def to_self(a, k):
                pl.when(which == 1)(lambda: go(a, k))

                @pl.when(which == 0)
                def _():
                    cols = pl.ds(pl.multiple_of(me * BLK, BLK), BLK)
                    orow[0, :, cols] = xpair[slot, me]

                    @pl.when(z < NZ // 2)
                    def _():
                        orow[1, :, cols] = xpair[slot, FULL // 2 + me]

            pl.when(wanted)(lambda: peers(go, to_self))
            return 0

        lax.fori_loop(0, n_out, each, 0)

    def pieces_out(slot, l):
        half = N // 2
        for which in range(n_out):
            @pl.when(table(l, lost_out if which else own_out) == 1)
            def _():
                if which:
                    landed(xpair.at[slot, pl.ds(0, N)], o_send.at[slot, which, 0])
                    landed(xpair.at[slot, pl.ds(0, half)], o_send.at[slot, which, 1])
                else:
                    landed(xpair.at[slot, pl.ds(0, N - 1)], o_send.at[slot, which, 0])
                    pl.when(z < NZ // 2)(lambda: landed(xpair.at[slot, pl.ds(0, half - 1)], o_send.at[slot, which, 1]))
                    pl.when(z >= NZ // 2)(lambda: landed(xpair.at[slot, pl.ds(0, half)], o_send.at[slot, which, 1]))

    def row_copy(part, a, k):
        dx, dy = XY[k]
        zz = shifted(table(a, SEND_DZ))
        first = zz * NXY + xs_of[dx] * NY + ys[dy] + (FULL // 2 if part else 0)
        return pltpu.make_async_remote_copy(
            src_ref=prow.at[first], dst_ref=rrow.at[part, (NZ - 1 - a) * NXY + XY_BACK[k]],
            send_sem=p_send.at[part], recv_sem=p_recv.at[part, NZ - 1 - a],
            device_id=(sec, zz, xs_of[dx], ys[dy]), device_id_type=MESH_ID,
        )

    def finish_rows():
        with scope("rowsend"):
            def short_rows(a, k):
                pl.when(shifted(table(a, SEND_DZ)) < NZ // 2)(lambda: row_copy(1, a, k).start())

            peers(short_rows)
            peers(lambda a, k: row_copy(0, a, k).start())
        with scope("rowpick"):
            r = lax.broadcasted_iota(jnp.int32, (8, ROWS), 0)
            c = lax.broadcasted_iota(jnp.int32, (8, ROWS), 1)
            pick = jnp.where(c == me * 2 + jnp.where(r < 2, r, r - 2 + FULL), 1.0, 0.0)
            pick = jnp.where((r < 2) | (z < NZ // 2), pick, 0.0).astype(jnp.bfloat16)

            def fetch(i, _):
                cols = pl.ds(pl.multiple_of(shifted(table(i, TAKE_DZ)) * (NXY * BLK), NXY * BLK), NXY * BLK)
                x = jnp.concatenate([xbuf[1, i * NXY + k].reshape(ROWS, BLK) for k in range(NXY)], axis=1)
                xrow[:, cols] = jnp.dot(pick, x, preferred_element_type=jnp.float32)
                return 0

            lax.fori_loop(0, NZ, fetch, 0)
            rrow[0, N // NZ - 1] = prow[me]

            @pl.when(z < NZ // 2)
            def _():
                rrow[1, N // NZ - 1] = prow[FULL // 2 + me]

        def total_of(part):
            def take(i, total):
                pl.when(i == 0)(lambda: landed(rrow.at[part, pl.ds(0, NXY - 1)], p_recv.at[part, 0]))
                pl.when(i > 0)(lambda: landed(rrow.at[part, pl.ds(i * NXY, NXY)], p_recv.at[part, i]))
                for k in range(NXY):
                    total += rrow[part, i * NXY + k].astype(jnp.float32)
                return total
            return lax.fori_loop(0, NZ, take, jnp.zeros((2, N * BLK), jnp.float32))

        with scope("rowsum"):
            orow[0] = (xrow[0:2, :] + total_of(0)).astype(jnp.bfloat16)

            @pl.when(z < NZ // 2)
            def _():
                r = lax.broadcasted_iota(jnp.int32, (2, 1), 0) + me * 2
                orow[1] = (xrow[2:4, :] + jnp.where(r < short_count, 1.0, 0.0) * total_of(1)).astype(jnp.bfloat16)

    def half_block(half, src, to, recv):
        return pltpu.make_async_remote_copy(
            src_ref=hbuf.at[src, half], dst_ref=hbuf.at[src, half], send_sem=h_send.at[0], recv_sem=recv,
            device_id=(sec, *to), device_id_type=MESH_ID,
        )

    def along_z(src):
        for d in (2, 1, 3):
            half_block(0, src, (zs[d], xh, y), h2_recv.at[0, (-d) % NZ]).start()

    def along_y(src):
        for d in (2, 1, 3):
            half_block(1, src, (z, xh, ys[d]), h2_recv.at[1, (-d) % NY]).start()

    def gathered_down(hidden):
        hbuf[me] = hidden.reshape(2, ROWS // 2, UNITS)
        with scope("hsend"):
            for k in range(NXY - 1):
                dx, dy = XY[k]
                half_block(0, me, (z, xs_of[dx], ys[dy]), h1_recv.at[0, XY_BACK[k]]).start()
                dz, dx = ZX[k]
                half_block(1, me, (zs[dz], xs_of[dx], y), h1_recv.at[1, ZX_BACK[k]]).start()
            along_z(me)
            along_y(me)
        with scope("hforward"):
            for k in range(NXY - 2, -1, -1):
                dx, dy = XY[k]
                src = z * NXY + xs_of[dx] * NY + ys[dy]
                landed(hbuf.at[src, 0], h1_recv.at[0, k])
                along_z(src)
                dz, dx = ZX[k]
                src = zs[dz] * NXY + xs_of[dx] * NY + y
                landed(hbuf.at[src, 1], h1_recv.at[1, k])
                along_y(src)
        with scope("hwait"):
            for half in range(2):
                for d in (1, 3, 2):
                    landed(hbuf.at[pl.ds(0, NXY), half], h2_recv.at[half, d])
        tot[...] = jnp.zeros_like(tot)

        def take(i, _):
            with scope("hdown"):
                landed(wd.at[0, pl.ds(i * NXY, NXY)], wd_sem.at[0, i])
                total = tot[...].reshape(ROWS, BLK)
                for k in range(NXY):
                    units = hbuf[i * NXY + k].reshape(ROWS, UNITS)
                    block = jnp.dot(units, wd[0, i * NXY + k], preferred_element_type=jnp.float32)
                    total += block.astype(jnp.bfloat16).astype(jnp.float32)
                tot[...] = total.reshape(2, HALF, BLK)
            return 0

        lax.fori_loop(0, NZ, take, 0)

    def gate_up(slot, l, n):
        pair = (NZ - 1 - n,)

        @pl.when(l > 0)
        def _():
            for i in pair:
                short = (i == 0) & (slot == 1) & runs_moved

                @pl.when(short)
                def _():
                    landed(xbuf.at[slot, pl.ds(0, NXY - 1)], ag_recv.at[slot, 0])

                @pl.when(jnp.logical_not(short))
                def _():
                    landed(xbuf.at[slot, pl.ds(i * NXY, NXY)], ag_recv.at[slot, i])

        def add(turned):
            squares = ssq[...]
            gate, up = accg[...], accu[...]
            which = lax.broadcasted_iota(jnp.int32, (4, 1), 0)
            for i in pair:
                cols = pl.ds(pl.multiple_of(shifted(table(i, TAKE_DZ)) * (NXY * BLK), NXY * BLK), NXY * BLK)
                gain = jnp.sum(jnp.where(which == l, gain_v[:, cols].astype(jnp.float32), 0.0), axis=0, keepdims=True)
                parts = []
                for k in range(NXY):
                    xf = xbuf[slot, i * NXY + k].reshape(ROWS, BLK).astype(jnp.float32)
                    squares += xf * xf
                    parts.append((xf * gain[:, k * BLK:(k + 1) * BLK]).astype(jnp.bfloat16))
                lhs = jnp.concatenate(parts, axis=1)
                weights = wgt if turned else wg
                dims = (((1,), (0 if turned else 1,)), ((), ()))
                gate += lax.dot_general(lhs, weights[slot, i, 0], dims, preferred_element_type=jnp.float32)
                up += lax.dot_general(lhs, weights[slot, i, 1], dims, preferred_element_type=jnp.float32)
            ssq[...] = squares
            accg[...] = gate
            accu[...] = up

        pl.when(turns)(lambda: add(True))

        @pl.when(jnp.logical_not(turns))
        def _():
            for i in pair:
                landed(wg.at[slot, i], wg_sem.at[slot, i])
            add(False)

    def layer(slot, _):
        l = sec - 1 + slot
        to_group = table(l, next_group)
        to_slot = table(l, next_slot)
        stays = to_group == sec

        @pl.when(jnp.where(slot == 0, runs_moved, runs_own))
        def _():
            accg[...] = jnp.zeros_like(accg)
            accu[...] = jnp.zeros_like(accu)
            ssq[...] = jnp.zeros_like(ssq)
            def step(i, _):
                with scope("gu"):
                    gate_up(slot, l, i)
                return 0

            lax.fori_loop(0, NZ, step, 0)
            with scope("hid"):
                mean = jnp.sum(ssq[...], axis=1, keepdims=True) * (1.0 / (N * BLK))
                scale = lax.rsqrt(mean + NORM_EPS)
                gate = accg[...] * scale
                hidden = (gate / (1.0 + jnp.exp(-gate)) * (accu[...] * scale)).astype(jnp.bfloat16)
            pl.when(l == 0)(meet)
            def down(a, _):
                with scope("down"):
                    landed(wd.at[slot, pl.ds(a * NXY, NXY)], wd_sem.at[slot, a])
                    w = jnp.concatenate([wd[slot, a * NXY + k] for k in range(NXY)], axis=1)
                    part = jnp.dot(hidden, w, preferred_element_type=jnp.float32).astype(jnp.bfloat16)

                    @pl.when(l < 3)
                    def _():
                        for k in range(NXY):
                            for half in range(2):
                                ps[slot, half, a * NXY + k] = part[half * HALF:(half + 1) * HALF, k * BLK:(k + 1) * BLK]
                        for k in range(NXY - 1):
                            rs_copy(slot, 0, a, k).start()
                        pl.when(a < NZ - 1)(lambda: rs_copy(slot, 0, a, NXY - 1).start())

                    @pl.when(l == 3)
                    def _():
                        zz = shifted(table(a, SEND_DZ))
                        for k, (dx, dy) in enumerate(XY):
                            cols = pl.ds(pl.multiple_of((zz * NXY + xs_of[dx] * NY + ys[dy]) * BLK, BLK), BLK)
                            prow[:, :, cols] = part[:, k * BLK:(k + 1) * BLK].reshape(ROWS // 2, 2, BLK)
                return 0

            def reduced_down():
                lax.fori_loop(0, NZ, down, 0)

                @pl.when(l < 3)
                def _():
                    peers(lambda a, k: rs_copy(slot, 1, a, k).start())
                    for half in range(2):
                        rs[slot, half, NXY - 1] = ps[slot, half, N - 1]

            by_units = gathers & (slot == 0)
            if any_gather:
                pl.when(by_units)(lambda: gathered_down(hidden))
                pl.when(jnp.logical_not(by_units))(reduced_down)
            else:
                reduced_down()

            def pass_on(half, _):
                @pl.when(jnp.logical_not(by_units))
                def _():
                    def take(i, total):
                        pl.when(i == 0)(lambda: landed(rs.at[slot, half, pl.ds(0, NXY - 1)], rs_recv.at[slot, half, 0]))
                        pl.when(i > 0)(lambda: landed(rs.at[slot, half, pl.ds(i * NXY, NXY)], rs_recv.at[slot, half, i]))
                        for k in range(NXY):
                            total += rs[slot, half, i * NXY + k].astype(jnp.float32)
                        return total

                    with scope("sum"):
                        tot[half] = lax.fori_loop(0, NZ, take, jnp.zeros((HALF, BLK), jnp.float32))

                row = lax.broadcasted_iota(jnp.int32, (HALF, 1), 0) + half * HALF
                keep = jnp.where(row < FULL + short_count, 1.0, 0.0)
                new = (xbuf[slot, xy, half].astype(jnp.float32) + keep * tot[half]).astype(jnp.bfloat16)
                xs[slot, half] = new

                @pl.when(stays)
                def _():
                    xbuf[1, xy, half] = new

                def send(copy):
                    def at_home(a, k):
                        pl.when(jnp.logical_not(stays))(lambda: copy(a, k).start())

                    peers(lambda a, k: copy(a, k).start(), at_home)

                with scope("ag"):
                    if any_gather:
                        pl.when(jnp.logical_not(by_units))(
                            lambda: send(lambda a, k: ag_copy(slot, half, to_group, to_slot, a, k))
                        )
                        pl.when(by_units & (half == 1))(
                            lambda: send(lambda a, k: ag_whole(slot, to_group, to_slot, a, k))
                        )
                    else:
                        send(lambda a, k: ag_copy(slot, half, to_group, to_slot, a, k))
                xpair[slot, pl.ds(half * (HALF // 2), HALF // 2)] = new.reshape(HALF // 2, 2, BLK)
                return 0

            @pl.when(l < 3)
            def _():
                lax.fori_loop(0, 2, pass_on, 0)
                with scope("pieces"):
                    pieces(slot, l)

            pl.when(l == 3)(finish_rows)
        return 0

    lax.fori_loop(0, 2, layer, 0)
    pl.when(sec == runs[0])(find_kept)

    comes = table(sec, source)
    with scope("rows"):
        for part in (0, 1):
            def wait_rows(count):
                landed(orow.at[part, :, pl.ds(0, count * BLK)], o_recv.at[part])

            here = (comes >= 0) & (sec < 3)
            if part:
                here = here & (z < NZ // 2)
            pl.when(here & (comes == sec))(lambda: wait_rows(N - 1))
            pl.when(here & (comes != sec))(lambda: wait_rows(N))

    @pl.when(comes < 0)
    def _():
        orow[0] = kept[0]

    @pl.when((comes < 0) | (z >= NZ // 2))
    def _():
        orow[1] = kept[1]

    with scope("assemble"):
        touched_full = comes >= 0
        touched_short = (comes >= 0) & (z < NZ // 2)
        for b in range(2):
            computed = jnp.where(full == b, orow[0].astype(jnp.float32), orow[1].astype(jnp.float32))
            use = jnp.where(full == b, jnp.where(touched_full, 1, 0), jnp.where(touched_short, 1, 0)) == 1
            out_ref[b] = jnp.where(use, computed, kept[b].astype(jnp.float32)).astype(jnp.bfloat16)

    def drain(slot, _):
        l = sec - 1 + slot
        to_group = table(l, next_group)
        to_slot = table(l, next_slot)
        stays = to_group == sec

        @pl.when(jnp.where(slot == 0, runs_moved, runs_own))
        def _():
            by_units = gathers & (slot == 0)
            pl.when(by_units)(lambda: landed(hbuf.at[pl.ds(0, N - 1)], h_send.at[0]))

            @pl.when(l < 3)
            def _():
                @pl.when(jnp.logical_not(by_units))
                def _():
                    for half in range(2):
                        sent = ps.at[slot, half, pl.ds(0, N - 1)]
                        landed(sent, rs_send.at[slot, half])
                        pl.when(stays)(lambda: landed(sent, ag_send.at[slot, half]))
                        pl.when(jnp.logical_not(stays))(lambda: landed(ps.at[slot, half], ag_send.at[slot, half]))

                @pl.when(by_units)
                def _():
                    pl.when(stays)(lambda: landed(xbuf.at[slot, pl.ds(0, N - 1)], ag_send.at[slot, 1]))
                    pl.when(jnp.logical_not(stays))(lambda: landed(xbuf.at[slot], ag_send.at[slot, 1]))

                pieces_out(slot, l)

            @pl.when(l == 3)
            def _():
                landed(prow.at[pl.ds(0, N - 1)], p_send.at[0])
                pl.when(z < NZ // 2)(lambda: landed(prow.at[pl.ds(0, N // 2 - 1)], p_send.at[1]))
                pl.when(z >= NZ // 2)(lambda: landed(prow.at[pl.ds(0, N // 2)], p_send.at[1]))
        return 0

    with scope("drain"):
        lax.fori_loop(0, 2, drain, 0)
        pl.when(spreads)(lambda: landed(wd.at[0, pl.ds(0, N - 1)], rd_send.at[0]))


def relay(moved, counts, tokens, gains, w_in, w_out, b_in, b_out):
    bf, f32 = jnp.bfloat16, jnp.float32
    dma = pltpu.SemaphoreType.DMA
    anywhere = pl.BlockSpec(memory_space=pl.ANY)
    return pl.pallas_call(
        functools.partial(relay_kernel, moved),
        out_shape=jax.ShapeDtypeStruct((2, 2, N * BLK), bf),
        in_specs=[pl.BlockSpec(memory_space=pltpu.SMEM)] + [anywhere] * 6,
        out_specs=pl.BlockSpec(memory_space=pltpu.VMEM),
        scratch_shapes=[
            pltpu.VMEM((2, FULL, N * BLK), bf),
            pltpu.VMEM((4, N * BLK), bf),
            pltpu.VMEM((2, NZ, 2, UNITS, NXY * BLK), bf),
            pltpu.VMEM((2, NZ, 2, NXY * BLK, UNITS), bf),
            pltpu.VMEM((2, N, UNITS, BLK), bf),
            pltpu.VMEM((2, N, 2, HALF, BLK), bf),
            pltpu.VMEM((2, 2, N, HALF, BLK), bf),
            pltpu.VMEM((2, 2, N, HALF, BLK), bf),
            pltpu.VMEM((2, 2, HALF, BLK), bf),
            pltpu.VMEM((2, ROWS // 2, 2, BLK), bf),
            pltpu.VMEM((2, 2, N * BLK), bf),
            pltpu.VMEM((2, 2, N * BLK), bf),
            pltpu.VMEM((ROWS, UNITS), f32),
            pltpu.VMEM((ROWS, UNITS), f32),
            pltpu.VMEM((ROWS, BLK), f32),
            pltpu.VMEM((2, HALF, BLK), f32),
            pltpu.VMEM((ROWS // 2, 2, N * BLK), bf),
            pltpu.VMEM((2, N, 2, N * BLK), bf),
            pltpu.VMEM((8, N * BLK), f32),
            pltpu.VMEM((N, 2, ROWS // 2, UNITS), bf),
            dma((2,)),
            dma((2, NZ)),
            dma((2, NZ)),
            dma((1,)),
            dma((2, 2)),
            dma((2, 2, NZ)),
            dma((2, 2)),
            dma((2, NZ)),
            dma((2, 2, 2)),
            dma((2,)),
            dma((2,)),
            dma((2, NZ)),
            dma((1,)),
            dma((2, NXY)),
            dma((2, NZ)),
        ],
        compiler_params=pltpu.CompilerParams(
            collective_id=PLANS.index(moved), has_side_effects=True, vmem_limit_bytes=60 * 1024 * 1024
        ),
    )(counts, tokens, gains, w_in, w_out, b_in, b_out)


def shards(tokens, norm_gain, w_in, w_out, backup_in, backup_out, layer_group, token_counts):
    unmoved = sum(w * l for l, w in enumerate(PLAN_WEIGHTS))
    plan = jnp.sum(layer_group * jnp.array(PLAN_WEIGHTS, jnp.int32)) - (unmoved + 1)
    rows = lax.switch(
        plan,
        [functools.partial(relay, p) for p in PLANS],
        token_counts, tokens, norm_gain, w_in[0], w_out[0], backup_in[0], backup_out[0],
    )
    return rows[None]


def solution(mesh):
    finer = Mesh(mesh.devices.reshape(4, NZ, NX, NY), AXES)
    return jax.shard_map(
        shards,
        mesh=finer,
        in_specs=(
            P(),
            P(),
            P("section", None, TENSOR, None),
            P("section", TENSOR, None),
            P("section", None, TENSOR, None),
            P("section", None, TENSOR),
            P(),
            P(),
        ),
        out_specs=P("section", None, TENSOR, None),
        check_vma=False,
    )
```
